32 devices in a mesh: req: 8 (over z, x), seq: 4 (over y, core).
Axes of the slice: x: 2, y: 2, z: 4, core: 2. Of those that a mesh axis runs over, the one named last changes fastest.
Arguments:
- pool_states: float32 [104, 64, 64, 128], P('req', 'seq'), may hold values from -6 to 6
- inner_window: bfloat16 [104, 3, 4096], P('req', None, 'seq'), may hold values from -6 to 6
- state_window: bfloat16 [104, 3, 256], P('req', None, 'seq'), may hold values from -6 to 6
- move_plan: int32 [104, 2], P('req'), may hold values from 0 to 12, as said below
- active_mask: int32 [104], P('req'), may hold values 0 or 1
- inputs_inner: bfloat16 [8, 2048, 4096], P('req', 'seq'), may hold values from -6 to 6
- inputs_state: bfloat16 [8, 2048, 256], P('req', 'seq'), may hold values from -6 to 6
- gate_rows: bfloat16 [8, 2048, 4096], P('req', 'seq'), may hold values from -6 to 6
- step_raw: bfloat16 [8, 2048, 64], P('req', 'seq'), may hold values from -8 to 60
- lengths: int32 [8], P('req'), may hold values from 4 to 2048
- conv_weight: float32 [4, 4352], replicated, may hold values from -3 to 3
- conv_bias: float32 [4352], replicated, may hold values from -3 to 3
- step_bias: float32 [64], replicated, may hold values from -3.3 to -2.7
- decay_log: float32 [64], replicated, may hold values from -10 to 0
- skip_weight: float32 [64], replicated, may hold values from 0.5 to 1.5
- norm_weight: float32 [4096], replicated, may hold values from 0.25 to 1.75
Outputs:
- new_states: float32 [104, 64, 64, 128], P('req', 'seq')
- new_inner_window: bfloat16 [104, 3, 4096], P('req', None, 'seq')
- new_state_window: bfloat16 [104, 3, 256], P('req', None, 'seq')
- mixer_out: bfloat16 [8, 2048, 4096], P('req', 'seq')
The draws below stay inside these ranges and needn't reach their ends.
Inputs may be any that keep to these rules, and one draw needn't show every extreme that they name: `move_plan`: every pair of a destination index along req and a slot 0 .. 12 is named exactly once; the rows of one device name one destination at most 4 times, and some destination exactly 4 times.
All inputs are finite; a program needn't handle non-finite values. No bound on the sum of `active_mask` on one device may be relied on, other than what follows from the above.
Results may differ from the reference program's by a relative error of at most 0.0087.
Values may be sent and summed in bfloat16 or wider, within the bound.
A program may use at most 192 MiB of HBM per device.

```python
import jax
import jax.numpy as jnp
from jax import lax

HEAD_COUNT = 64
HEAD_DIM = 64
STATE_DIM = 128
KERNEL = 4
BLOCK_LEN = 256
SLOTS_DEV = 13
PREFILLS = 1
INNER_DIM = 4096
CHANNELS = 4352
CAPACITY = 4
PROMPT_SPAN = 2048
PROMPT_TOTAL = 8
POOL_SLOTS = 104


def draw_move_plan(key, part):
    peer_count = POOL_SLOTS // SLOTS_DEV
    sampler_seeds = jax.random.split(jax.random.fold_in(key, 11), 5)
    outer_order = jax.random.permutation(sampler_seeds[0], peer_count)
    inner_order = jax.random.permutation(sampler_seeds[1], peer_count)
    slot_order = jax.random.permutation(sampler_seeds[2], SLOTS_DEV)
    rotation = jax.random.randint(sampler_seeds[3], (), 0, peer_count)
    offsets = ((jnp.arange(SLOTS_DEV) // CAPACITY + rotation) % peer_count)[slot_order]
    devices = jnp.arange(peer_count)
    target_device = outer_order[(inner_order[devices][:, None] + offsets[None, :]) % peer_count]

    def slot_table(table_key):
        return jax.random.permutation(table_key, SLOTS_DEV)
    slot_tables = jax.vmap(slot_table)(jax.random.split(sampler_seeds[4], peer_count))
    target_slot = slot_tables[target_device, jnp.arange(SLOTS_DEV)[None, :]]
    return jnp.stack([target_device, target_slot], axis=-1).reshape(POOL_SLOTS, 2).astype(jnp.int32)


def draw_step_raw(key, part):
    sampler_seeds = jax.random.split(jax.random.fold_in(key, 23), 4)
    blocks = PROMPT_SPAN // BLOCK_LEN
    offset_steps = jax.random.uniform(sampler_seeds[0], (PROMPT_TOTAL, blocks, 1, HEAD_COUNT), minval=-0.8, maxval=0.8)
    offset_steps = jnp.broadcast_to(offset_steps, (PROMPT_TOTAL, blocks, BLOCK_LEN, HEAD_COUNT)).reshape(PROMPT_TOTAL, PROMPT_SPAN, HEAD_COUNT)
    jitter_addend = 0.7 * jax.random.normal(sampler_seeds[1], (PROMPT_TOTAL, PROMPT_SPAN, HEAD_COUNT))
    arrival_tallies = jax.random.uniform(sampler_seeds[2], (PROMPT_TOTAL, PROMPT_SPAN, 1)) < 3.0 / PROMPT_SPAN
    level_entries = jax.random.uniform(sampler_seeds[3], (PROMPT_TOTAL, PROMPT_SPAN, HEAD_COUNT), minval=34.0, maxval=46.0)
    payload_array = offset_steps + jitter_addend + jnp.where(arrival_tallies, level_entries, 0.0)
    return jnp.clip(payload_array, -8.0, 60.0).astype(jnp.float32).astype(jnp.bfloat16)


def draw_decay_log(key, part):
    sampler_seeds = jax.random.split(jax.random.fold_in(key, 37), 3)
    slow_low = jnp.log(0.5 / (0.05 * PROMPT_SPAN))
    slow_high = jnp.log(2.0 / (0.05 * PROMPT_SPAN))
    fast_share = 0.5
    slow_part = jax.random.uniform(sampler_seeds[0], (HEAD_COUNT,), minval=slow_low, maxval=slow_high)
    fast_part = jax.random.uniform(sampler_seeds[1], (HEAD_COUNT,), minval=jnp.log(0.3), maxval=jnp.log(0.67))
    fast_pick = jax.random.uniform(sampler_seeds[2], (HEAD_COUNT,)) < fast_share
    return jnp.where(fast_pick, fast_part, slow_part).astype(jnp.float32)


def plant(drawn, stream_key, low, largest):
    longest = drawn.shape.index(max(drawn.shape))
    spots = []
    for shift in (0, 1):
        where = [jax.random.randint(jax.random.fold_in(stream_key, axis), (), 0, length) for axis, length in enumerate(drawn.shape)]
        where[longest] = (where[longest] + shift) % drawn.shape[longest]
        spots.append(tuple(where))
    return drawn.at[spots[0]].set(low).at[spots[1]].set(largest)


def block_scale(own_key, shape, shards, least, high):
    level = 1.0
    for dim, blocks in shards:
        draws = jax.random.uniform(jax.random.fold_in(jax.random.fold_in(own_key, 6), dim), (blocks,), jnp.float32, least / len(shards), high / len(shards))
        level = level * jnp.repeat(jnp.exp(draws), shape[dim] // blocks).reshape((-1,) + (1,) * (len(shape) - 1 - dim))
    return level


def normal_values(own_key, dims, width, limit, pieces=(), kind=jnp.bfloat16):
    entries = jax.random.normal(own_key, dims, jnp.float32) * width
    if len(pieces) > 0:
        entries = block_scale(own_key, dims, pieces, -0.22, 0.18) * entries
    return jnp.clip(entries, min=-limit, max=limit).astype(kind)


def setup_inputs(seed: int = 0) -> dict:
    streams_of = jax.random.split(jax.random.key(seed), 17)
    pool_states = normal_values(streams_of[0], (POOL_SLOTS, HEAD_COUNT, HEAD_DIM, STATE_DIM), 1.0, 6.0, ((0, 8), (1, 4)), jnp.float32)
    inner_window = normal_values(streams_of[1], (POOL_SLOTS, KERNEL - 1, INNER_DIM), 1.0, 6.0, ((0, 8), (2, 4)))
    state_window = normal_values(streams_of[2], (POOL_SLOTS, KERNEL - 1, 2 * STATE_DIM), 1.0, 6.0, ((0, 8), (2, 4)))
    move_plan = draw_move_plan(jax.random.fold_in(streams_of[16], 71), 0)
    active_mask = plant((jax.random.randint(streams_of[4], (POOL_SLOTS,), 0, 4) < 3).astype(jnp.int32), jax.random.fold_in(streams_of[4], 1), 0, 1)
    inputs_inner = normal_values(streams_of[5], (PROMPT_TOTAL, PROMPT_SPAN, INNER_DIM), 1.0, 6.0, ((0, 8), (1, 4)))
    inputs_state = normal_values(streams_of[6], (PROMPT_TOTAL, PROMPT_SPAN, 2 * STATE_DIM), 1.0, 6.0, ((0, 8), (1, 4)))
    gate_rows = normal_values(streams_of[7], (PROMPT_TOTAL, PROMPT_SPAN, INNER_DIM), 1.0, 6.0, ((0, 8), (1, 4)))
    step_raw = draw_step_raw(jax.random.fold_in(streams_of[16], 71), 0)
    lengths = plant(jax.random.randint(streams_of[9], (PROMPT_TOTAL,), KERNEL, PROMPT_SPAN + 1), jax.random.fold_in(streams_of[9], 1), KERNEL, PROMPT_SPAN).astype(jnp.int32)
    conv_weight = normal_values(streams_of[10], (KERNEL, CHANNELS), KERNEL ** -0.5, 3.0, (), jnp.float32)
    conv_bias = normal_values(streams_of[11], (CHANNELS,), 0.5, 3.0, (), jnp.float32)
    step_bias = jnp.clip(jax.random.uniform(streams_of[12], (HEAD_COUNT,), jnp.float32, -3.3, -2.7), -3.3, -2.7)
    decay_log = draw_decay_log(jax.random.fold_in(streams_of[16], 71), 0)
    skip_weight = jnp.clip(jax.random.uniform(streams_of[14], (HEAD_COUNT,), jnp.float32, 0.5, 1.5), 0.5, 1.5)
    norm_weight = jnp.clip(1.0 + 0.15 * jax.random.normal(streams_of[15], (INNER_DIM,), jnp.float32), 0.25, 1.75)
    return dict(pool_states=pool_states, inner_window=inner_window, state_window=state_window, move_plan=move_plan, active_mask=active_mask, inputs_inner=inputs_inner, inputs_state=inputs_state, gate_rows=gate_rows, step_raw=step_raw, lengths=lengths, conv_weight=conv_weight, conv_bias=conv_bias, step_bias=step_bias, decay_log=decay_log, skip_weight=skip_weight, norm_weight=norm_weight)


EPSILON = 1e-05

def conv_silu(window, new_rows, weight, bias_values):
    extended = jnp.concatenate([window, new_rows], axis=1).astype(jnp.float32)
    length = new_rows.shape[1]
    running = jnp.zeros(new_rows.shape, jnp.float32) + bias_values
    for offset in range(weight.shape[0]):
        running = running + weight[offset] * extended[:, offset:offset + length]
    return jax.nn.silu(running).astype(jnp.bfloat16)

def block_local(value_rows, write_rows, read_rows, step_rows, decay_rates):
    log_decay = step_rows * decay_rates
    running_log = jnp.cumsum(log_decay, axis=0)
    scores = jnp.dot(read_rows, write_rows.T, preferred_element_type=jnp.float32)
    log_heads = running_log.T
    log_gaps = log_heads[:, :, None] - log_heads[:, None, :]
    positions = jnp.arange(running_log.shape[0])
    causal = positions[:, None] >= positions[None, :]
    decays = jnp.where(causal, jnp.exp(jnp.where(causal, log_gaps, 0.0)), 0.0)
    weights = (scores[None] * decays * step_rows.T[:, None, :]).astype(jnp.bfloat16)
    intra_part = jnp.einsum('hts,shp->thp', weights.astype(jnp.float32), value_rows.astype(jnp.float32))
    to_end = jnp.exp(running_log[-1:] - running_log) * step_rows
    scaled = (to_end[:, :, None] * value_rows.astype(jnp.float32)).astype(jnp.bfloat16)
    block_state = jnp.einsum('shp,sn->hpn', scaled.astype(jnp.float32), write_rows.astype(jnp.float32))
    return (intra_part, block_state, running_log)

def gated_norm(payload_array, gate_part, norm_weight):
    gated_rows = payload_array.astype(jnp.float32) * jax.nn.silu(gate_part.astype(jnp.float32))
    norm_scale = lax.rsqrt(lax.optimization_barrier(jnp.mean(gated_rows * gated_rows, axis=-1, keepdims=True)) + EPSILON)
    return (gated_rows * norm_scale * norm_weight).astype(jnp.bfloat16)

def reference(pool_states, inner_window, state_window, move_plan, active_mask, inputs_inner, inputs_state, gate_rows, step_raw, lengths, conv_weight, conv_bias, step_bias, decay_log, skip_weight, norm_weight):
    keep_flag = active_mask.astype(jnp.float32)
    targets = (move_plan[:, 0] * SLOTS_DEV + move_plan[:, 1]).astype(jnp.int32)
    moved_states = jnp.zeros_like(pool_states).at[targets].set(pool_states * keep_flag[:, None, None, None])
    moved_inner = jnp.zeros_like(inner_window).at[targets].set((inner_window.astype(jnp.float32) * keep_flag[:, None, None]).astype(jnp.bfloat16))
    moved_outer = jnp.zeros_like(state_window).at[targets].set((state_window.astype(jnp.float32) * keep_flag[:, None, None]).astype(jnp.bfloat16))
    sequence_index = jnp.arange(PROMPT_TOTAL).astype(jnp.int32)
    slot_index = (sequence_index // PREFILLS * SLOTS_DEV + sequence_index % PREFILLS).astype(jnp.int32)
    decay_rates = -jnp.exp(decay_log)
    block_count = PROMPT_SPAN // BLOCK_LEN

    def split_blocks(source):
        return source.reshape((block_count, BLOCK_LEN) + source.shape[1:])

    def one_block(members):
        return block_local(members[0], members[1], members[2], members[3], decay_rates)

    def advance(carried, members):
        block_state, running_log, read_block = members
        inter_part = jnp.einsum('qn,hpn->qhp', read_block.astype(jnp.float32), carried, precision=lax.Precision.HIGHEST) * jnp.exp(running_log)[:, :, None]
        updated = jnp.exp(running_log[-1])[:, None, None] * carried + block_state
        return (updated, inter_part)

    def prefill_one(members):
        initial, head_inner, head_outer, inner_rows, outer_rows, gate_part, step_part, length_one = members
        raw_rows = jnp.concatenate([inner_rows, outer_rows], axis=1)
        window = jnp.concatenate([head_inner, head_outer], axis=1)
        mixed_rows = conv_silu(window[None], raw_rows[None], conv_weight, conv_bias)[0]
        value_rows = mixed_rows[:, :INNER_DIM].reshape(PROMPT_SPAN, HEAD_COUNT, HEAD_DIM)
        write_rows = mixed_rows[:, INNER_DIM:INNER_DIM + STATE_DIM]
        read_rows = mixed_rows[:, INNER_DIM + STATE_DIM:]
        valid_rows = (jnp.arange(PROMPT_SPAN).astype(jnp.int32) < length_one).astype(jnp.float32)
        step_sizes = jax.nn.softplus(step_part.astype(jnp.float32) + step_bias) * valid_rows[:, None]
        intra_part, block_states, running_logs = lax.map(one_block, (split_blocks(value_rows), split_blocks(write_rows), split_blocks(read_rows), split_blocks(step_sizes)))
        final_state, inter_parts = lax.scan(advance, initial, (block_states, running_logs, split_blocks(read_rows)))
        combined = (intra_part + inter_parts).reshape(PROMPT_SPAN, HEAD_COUNT, HEAD_DIM) + skip_weight[:, None] * value_rows.astype(jnp.float32)
        y_rows = (combined * valid_rows[:, None, None]).astype(jnp.bfloat16).reshape(PROMPT_SPAN, INNER_DIM)
        mixer_rows = gated_norm(y_rows, gate_part, norm_weight)
        window_pos = (length_one - (KERNEL - 1) + jnp.arange(KERNEL - 1)).astype(jnp.int32)
        last_window = jnp.take(raw_rows, window_pos, axis=0)
        return (final_state, last_window, mixer_rows)
    final_states, last_windows, mixer_out = lax.map(prefill_one, (moved_states[slot_index], moved_inner[slot_index], moved_outer[slot_index], inputs_inner, inputs_state, gate_rows, step_raw, lengths))
    new_states = moved_states.at[slot_index].set(final_states)
    new_inner = moved_inner.at[slot_index].set(last_windows[:, :, :INNER_DIM])
    new_outer = moved_outer.at[slot_index].set(last_windows[:, :, INNER_DIM:])
    return (new_states, new_inner, new_outer, mixer_out)
```

```python
import functools

import jax
import jax.numpy as jnp
from jax import lax
from jax.experimental import pallas as pl
from jax.experimental.pallas import tpu as pltpu
from jax.sharding import PartitionSpec as P

HEAD_DIM = 64
STATE_DIM = 128
KERNEL = 4
BLOCK_LEN = 256
EPSILON = 1e-05
LANES = 128
HALO = 8
LOG2E = 1.4426950408889634
GROUP = 2 * LANES


def half_silu(v):
    return (0.5 * v) * (1.0 + jnp.tanh(0.5 * v))


def conv_rows(ext_ref, weight_ref, bias_ref, start, count):
    total = bias_ref[...] + weight_ref[KERNEL - 1 : KERNEL, :] * ext_ref[pl.ds(start + HALO, count), :]
    for k in range(KERNEL - 1):
        total = total + weight_ref[k : k + 1, :] * ext_ref[pl.ds(start + HALO - KERNEL + 1 + k, count), :]
    return half_silu(total).astype(jnp.bfloat16)


def mix_kernel(
    nv_ref, x_ref, win_ref, cw_ref, cb_ref, skip_ref, xs_ref, wins_ref, cws_ref, cbs_ref, step_ref, sbias_ref, dlog_ref,
    part_ref, end_ref, ecum_ref, read_ref,
    ext, val, a_s, te_s, brow, write_t, score,
):
    g = pl.program_id(0)
    length = x_ref.shape[0]
    blocks = length // BLOCK_LEN
    half = BLOCK_LEN // 2

    @pl.when(g == 0)
    def _():
        ext[0:HALO, :] = wins_ref[...].astype(jnp.float32)
        ext[HALO : HALO + length, :] = xs_ref[...].astype(jnp.float32)
        ys = conv_rows(ext, cws_ref, cbs_ref, 0, length)
        write, read = ys[:, :STATE_DIM], ys[:, STATE_DIM:]
        read_ref[...] = read
        write_t[...] = write.astype(jnp.float32).T.astype(jnp.bfloat16)
        rows = lax.broadcasted_iota(jnp.int32, (length, LANES), 0)
        raw = step_ref[...] + sbias_ref[...]
        soft = jnp.maximum(raw, 0.0) + jnp.log1p(jnp.exp(-jnp.abs(raw)))
        dt = jnp.where(rows < nv_ref[0], soft, 0.0)
        rate = (dt * LOG2E) * (-jnp.exp(dlog_ref[...]))
        r = lax.broadcasted_iota(jnp.int32, (BLOCK_LEN, BLOCK_LEN), 0)
        c = lax.broadcasted_iota(jnp.int32, (BLOCK_LEN, BLOCK_LEN), 1)
        tri = (r >= c).astype(jnp.float32)
        before = jnp.zeros((1, LANES), jnp.float32)
        for blk in range(blocks):
            s = slice(blk * BLOCK_LEN, (blk + 1) * BLOCK_LEN)
            cum = jnp.dot(tri, rate[s], precision=lax.Precision.HIGHEST, preferred_element_type=jnp.float32)
            b = jnp.where(dt[s] > 0.0, cum - jnp.log2(dt[s]), 1e30)
            a_s[s, :] = cum
            last = cum[BLOCK_LEN - 1 : BLOCK_LEN, :]
            te_s[s, :] = jnp.exp2(last - b)
            brow[:, s] = b.T
            ecum_ref[s, :] = jnp.exp2(cum + before)
            before = before + last
            sc = lax.dot_general(read[s], write[s], (((1,), (1,)), ((), ())), preferred_element_type=jnp.float32)
            score[blk] = jnp.where(r >= c, sc, 0.0)

    ext[0:HALO, :] = win_ref[...].astype(jnp.float32)
    ext[HALO : HALO + length, :] = x_ref[...].astype(jnp.float32)
    rows_at_once = 64
    for i in range(length // rows_at_once):
        val[i * rows_at_once : (i + 1) * rows_at_once, :] = conv_rows(ext, cw_ref, cb_ref, i * rows_at_once, rows_at_once)

    heads_step = GROUP // HEAD_DIM
    turn = lax.rem(LANES - heads_step * g, LANES)
    a_all = pltpu.roll(a_s[...], turn, axis=1)
    te_all = pltpu.roll(te_s[...], turn, axis=1)
    low = lax.broadcasted_iota(jnp.int32, (1, LANES), 1) < HEAD_DIM

    for pair in range(GROUP // LANES):
        cols = slice(pair * LANES, (pair + 1) * LANES)
        skip = skip_ref[:, cols]
        before = None
        for blk in range(blocks):
            s = slice(blk * BLOCK_LEN, (blk + 1) * BLOCK_LEN)
            v = val[s, cols]
            vf = v.astype(jnp.float32)
            masked = [jnp.where(low, vf, 0.0).astype(jnp.bfloat16), jnp.where(low, 0.0, vf).astype(jnp.bfloat16)]
            tops, bottoms = [], []
            for j in range(2):
                h = 2 * pair + j
                a = a_all[s, h : h + 1]
                b = brow[pl.ds(heads_step * g + h, 1), s]
                top = jnp.exp2(jnp.minimum(a[:half] - b[:, :half], 126.0)) * score[blk, :half, :half]
                bot = jnp.exp2(jnp.minimum(a[half:] - b, 126.0)) * score[blk, half:, :]
                tops.append(top.astype(jnp.bfloat16))
                bottoms.append(bot.astype(jnp.bfloat16))
            intra_top = jnp.dot(
                jnp.concatenate(tops, axis=1), jnp.concatenate([m[:half] for m in masked], axis=0), preferred_element_type=jnp.float32
            )
            intra_bot = jnp.dot(
                jnp.concatenate(bottoms, axis=1), jnp.concatenate(masked, axis=0), preferred_element_type=jnp.float32
            )
            out = jnp.concatenate([intra_top, intra_bot], axis=0) + skip * vf
            h = 2 * pair
            te = jnp.where(low, te_all[s, h : h + 1], te_all[s, h + 1 : h + 2])
            state = jnp.dot(write_t[:, s], (te * vf).astype(jnp.bfloat16), preferred_element_type=jnp.float32)
            if blk > 0:
                e = jnp.exp2(jnp.where(low, a_all[s, h : h + 1], a_all[s, h + 1 : h + 2]))
                out = out + e * jnp.dot(read_ref[s, :], before.astype(jnp.bfloat16), preferred_element_type=jnp.float32)
                state = state + e[BLOCK_LEN - 1 : BLOCK_LEN, :] * before
            before = state
            part_ref[s, cols] = out.astype(jnp.bfloat16)
        end_ref[:, cols] = before.astype(jnp.bfloat16)


def mix(nv, x, xs, window, conv_weight, conv_bias, step_raw, step_bias, decay_log, skip_row):
    length, inner = x.shape
    pad = LANES - step_raw.shape[1]
    step = jnp.pad(step_raw.astype(jnp.float32), ((0, 0), (0, pad)))
    sbias = jnp.pad(step_bias, (0, pad))[None]
    dlog = jnp.pad(decay_log, (0, pad))[None]
    xs_width = xs.shape[1]
    fixed = lambda shape: pl.BlockSpec(shape, lambda i, nv: (0,) * len(shape))
    column = lambda rows: pl.BlockSpec((rows, GROUP), lambda i, nv: (0, i))
    blocks = length // BLOCK_LEN
    heads = inner // HEAD_DIM
    return pl.pallas_call(
        mix_kernel,
        grid_spec=pltpu.PrefetchScalarGridSpec(
            num_scalar_prefetch=1,
            grid=(inner // GROUP,),
            in_specs=[
                column(length), column(HALO), column(KERNEL), column(1), column(1),
                fixed((length, xs_width)), fixed((HALO, xs_width)), fixed((KERNEL, xs_width)), fixed((1, xs_width)),
                fixed((length, LANES)), fixed((1, LANES)), fixed((1, LANES)),
            ],
            out_specs=[column(length), column(STATE_DIM), fixed((length, LANES)), fixed((length, STATE_DIM))],
            scratch_shapes=[
                pltpu.VMEM((length + HALO, GROUP), jnp.float32),
                pltpu.VMEM((length, GROUP), jnp.bfloat16),
                pltpu.VMEM((length, LANES), jnp.float32),
                pltpu.VMEM((length, LANES), jnp.float32),
                pltpu.VMEM((LANES, length), jnp.float32),
                pltpu.VMEM((STATE_DIM, length), jnp.bfloat16),
                pltpu.VMEM((blocks, BLOCK_LEN, BLOCK_LEN), jnp.float32),
            ],
        ),
        out_shape=[
            jax.ShapeDtypeStruct((length, inner), jnp.bfloat16),
            jax.ShapeDtypeStruct((STATE_DIM, inner), jnp.bfloat16),
            jax.ShapeDtypeStruct((length, LANES), jnp.float32),
            jax.ShapeDtypeStruct((length, STATE_DIM), jnp.bfloat16),
        ],
        compiler_params=pltpu.CompilerParams(dimension_semantics=("arbitrary",)),
        cost_estimate=pl.CostEstimate(
            flops=2 * blocks * heads * BLOCK_LEN * BLOCK_LEN * LANES * 8,
            bytes_accessed=4 * length * inner, transcendentals=blocks * heads * BLOCK_LEN * BLOCK_LEN,
        ),
        name="mix",
    )(
        nv, x, window[:, :inner], conv_weight[:, :inner], conv_bias[None, :inner], skip_row,
        xs, window[:, inner:], conv_weight[:, inner:], conv_bias[None, inner:], step, sbias, dlog,
    )


CHUNK = 256


def finish_kernel(
    nv_ref, part_ref, gate_ref, read_ref, ecum_ref, ends_ref, coef_ref, init_ref, norm_ref, out_ref, prior, spread, gated
):
    step = pl.program_id(0)
    tile, inner = part_ref.shape
    chain = ends_ref.shape[0]
    heads = inner // HEAD_DIM

    @pl.when(step == 0)
    def _():
        def fill(i, carry):
            cols = pl.ds(pl.multiple_of(i * CHUNK, CHUNK), CHUNK)
            total = coef_ref[0:1, cols] * ends_ref[0, :, cols].astype(jnp.float32)
            for j in range(1, chain):
                total = total + coef_ref[j : j + 1, cols] * ends_ref[j, :, cols].astype(jnp.float32)
            prior[:, cols] = total.astype(jnp.bfloat16)
            k = lax.broadcasted_iota(jnp.int32, (LANES, CHUNK), 0)
            c = lax.broadcasted_iota(jnp.int32, (LANES, CHUNK), 1)
            owner = i * (CHUNK // HEAD_DIM) + c // HEAD_DIM
            spread[:, cols] = jnp.where((k == owner) | (k == owner + heads), 1.0, 0.0).astype(jnp.bfloat16)
            return carry

        lax.fori_loop(0, inner // CHUNK, fill, 0)

    read = read_ref[...]
    ecum = ecum_ref[...]
    first = ecum.astype(jnp.bfloat16).astype(jnp.float32)
    lane = lax.broadcasted_iota(jnp.int32, (tile, LANES), 1)
    both = jnp.where(lane < heads, first, pltpu.roll(ecum - first, heads, axis=1)).astype(jnp.bfloat16)
    rows = lax.broadcasted_iota(jnp.int32, (tile, 1), 0) + step * tile
    valid = (rows < nv_ref[0]).astype(jnp.float32)

    def gate_chunk(i, squares):
        cols = pl.ds(pl.multiple_of(i * CHUNK, CHUNK), CHUNK)
        z = jnp.dot(read, prior[:, cols], preferred_element_type=jnp.float32)
        zi = lax.dot_general(read, init_ref[cols, :], (((1,), (1,)), ((), ())), preferred_element_type=jnp.float32)
        e = jnp.dot(both, spread[:, cols], preferred_element_type=jnp.float32)
        z = z + coef_ref[chain : chain + 1, cols] * zi
        y = (part_ref[:, cols].astype(jnp.float32) + e * z) * valid
        y = y.astype(jnp.bfloat16).astype(jnp.float32)
        out = y * half_silu(gate_ref[:, cols].astype(jnp.float32))
        gated[:, cols] = out
        square = out * out
        for k in range(CHUNK // LANES):
            squares = squares + square[:, k * LANES : (k + 1) * LANES]
        return squares

    squares = lax.fori_loop(0, inner // CHUNK, gate_chunk, jnp.zeros((tile, LANES), jnp.float32))
    scale = lax.rsqrt(jnp.sum(squares, axis=1, keepdims=True) * (1.0 / inner) + EPSILON)

    def scale_chunk(i, carry):
        cols = pl.ds(pl.multiple_of(i * CHUNK, CHUNK), CHUNK)
        out_ref[:, cols] = (gated[:, cols] * scale * norm_ref[:, cols]).astype(jnp.bfloat16)
        return carry

    lax.fori_loop(0, inner // CHUNK, scale_chunk, 0)


def finish(nv, part, gate, read, ecum, ends, coef, initial, norm):
    length, inner = part.shape
    tile = min(128, length)
    chain = ends.shape[0]
    fixed = lambda shape: pl.BlockSpec(shape, lambda i, nv: (0,) * len(shape))
    row = lambda width: pl.BlockSpec((tile, width), lambda i, nv: (i, 0))
    return pl.pallas_call(
        finish_kernel,
        grid_spec=pltpu.PrefetchScalarGridSpec(
            num_scalar_prefetch=1,
            grid=(length // tile,),
            in_specs=[
                row(inner), row(inner), row(STATE_DIM), row(LANES),
                fixed(ends.shape), fixed(coef.shape), fixed(initial.shape), fixed((1, inner)),
            ],
            out_specs=row(inner),
            scratch_shapes=[
                pltpu.VMEM((STATE_DIM, inner), jnp.bfloat16),
                pltpu.VMEM((LANES, inner), jnp.bfloat16),
                pltpu.VMEM((tile, inner), jnp.float32),
            ],
        ),
        out_shape=jax.ShapeDtypeStruct((length, inner), jnp.bfloat16),
        compiler_params=pltpu.CompilerParams(dimension_semantics=("arbitrary",)),
        cost_estimate=pl.CostEstimate(
            flops=40 * length * inner * STATE_DIM // 8, bytes_accessed=6 * length * inner, transcendentals=length * inner
        ),
        name="finish",
    )(nv, part, gate, read, ecum, ends, coef, initial, norm)


def pack_kernel(keep_ref, state_ref, out_ref):
    keep = keep_ref[pl.program_id(0)].astype(jnp.float32)
    peers, _, rows, _ = out_ref.shape
    for i in range(peers):
        out_ref[i, 0] = (state_ref[0, i * rows : (i + 1) * rows] * keep).astype(out_ref.dtype)


def pack_pieces(states, keep, peers):
    slots, rows, lanes = states.shape
    piece = rows // peers
    return pl.pallas_call(
        pack_kernel,
        grid_spec=pltpu.PrefetchScalarGridSpec(
            num_scalar_prefetch=1,
            grid=(slots,),
            in_specs=[pl.BlockSpec((1, rows, lanes), lambda i, keep: (i, 0, 0))],
            out_specs=pl.BlockSpec((peers, 1, piece, lanes), lambda i, keep: (0, i, 0, 0)),
        ),
        out_shape=jax.ShapeDtypeStruct((peers, slots, piece, lanes), jnp.bfloat16),
        compiler_params=pltpu.CompilerParams(dimension_semantics=("arbitrary",)),
        cost_estimate=pl.CostEstimate(flops=slots * rows * lanes, bytes_accessed=6 * slots * rows * lanes, transcendentals=0),
        name="pack",
    )(keep, states)


def route_kernel(slots, source_ref, got_ref, first_ref, rest_ref):
    peers = first_ref.shape[0]

    def one_peer(d, carry):
        first_ref[d, 0] = got_ref[source_ref[d * slots]]
        for k in range(1, slots):
            rest_ref[d, k - 1] = got_ref[source_ref[d * slots + k]]
        return carry

    lax.fori_loop(0, peers, one_peer, 0)


def route(source, got, peers, slots):
    count, rows, lanes = got.shape
    return pl.pallas_call(
        functools.partial(route_kernel, slots),
        grid_spec=pltpu.PrefetchScalarGridSpec(
            num_scalar_prefetch=1,
            grid=(1,),
            in_specs=[pl.BlockSpec(got.shape, lambda i, s: (0, 0, 0))],
            out_specs=[
                pl.BlockSpec((peers, 1, rows, lanes), lambda i, s: (0, 0, 0, 0)),
                pl.BlockSpec((peers, slots - 1, rows, lanes), lambda i, s: (0, 0, 0, 0)),
            ],
        ),
        out_shape=[
            jax.ShapeDtypeStruct((peers, 1, rows, lanes), got.dtype),
            jax.ShapeDtypeStruct((peers, slots - 1, rows, lanes), got.dtype),
        ],
        compiler_params=pltpu.CompilerParams(dimension_semantics=("arbitrary",)),
        cost_estimate=pl.CostEstimate(flops=count * rows * lanes, bytes_accessed=4 * count * rows * lanes, transcendentals=0),
        name="route",
    )(source, got)


def place_kernel(final_ref, got_ref, out_ref):
    slot = pl.program_id(0)
    peers, _, rows, _ = got_ref.shape

    @pl.when(slot == 0)
    def _():
        out_ref[...] = final_ref[...]

    @pl.when(slot > 0)
    def _():
        for i in range(peers):
            out_ref[0, i * rows : (i + 1) * rows] = got_ref[i, 0].astype(out_ref.dtype)


def place(final, got):
    peers, rest, rows, lanes = got.shape
    slots = rest + 1
    return pl.pallas_call(
        place_kernel,
        grid=(slots,),
        in_specs=[
            pl.BlockSpec((1, peers * rows, lanes), lambda i: (0, 0, 0)),
            pl.BlockSpec((peers, 1, rows, lanes), lambda i: (0, jnp.maximum(i - 1, 0), 0, 0)),
        ],
        out_specs=pl.BlockSpec((1, peers * rows, lanes), lambda i: (i, 0, 0)),
        out_shape=jax.ShapeDtypeStruct((slots, peers * rows, lanes), jnp.float32),
        compiler_params=pltpu.CompilerParams(dimension_semantics=("arbitrary",)),
        cost_estimate=pl.CostEstimate(
            flops=slots * peers * rows * lanes, bytes_accessed=6 * slots * peers * rows * lanes, transcendentals=0
        ),
        name="place",
    )(final, got)


def exchange(source):
    return lax.all_to_all(source, "req", split_axis=0, concat_axis=0, tiled=True)


def on_device(
    pool_states, inner_window, state_window, move_plan, active_mask, inputs_inner, inputs_state, gate_rows, step_raw,
    lengths, conv_weight, conv_bias, step_bias, decay_log, skip_weight, norm_weight,
):
    peers, me = lax.axis_size("req"), lax.axis_index("req")
    chain, rank = lax.axis_size("seq"), lax.axis_index("seq")
    slots, heads_own = pool_states.shape[:2]
    length, inner = inputs_inner.shape[1:]
    own_width = inner_window.shape[2]
    states = pool_states.reshape(slots, -1, pool_states.shape[-1])
    rows = states.shape[1]

    got = exchange(pack_pieces(states, active_mask, peers))
    got = got.reshape((peers * slots,) + got.shape[2:])

    every_plan = lax.all_gather(move_plan, "req").reshape(-1, 2)
    target = every_plan[:, 0] * slots + every_plan[:, 1]
    order = jnp.arange(peers * slots, dtype=jnp.int32)
    source = jnp.sum(jnp.where(target[None, :] == order[:, None], order[None, :], 0), axis=1).astype(jnp.int32)

    windows = jnp.concatenate([inner_window, state_window], axis=2)
    windows = jnp.where(active_mask[:, None, None] != 0, windows, jnp.zeros_like(windows))
    every_window = lax.all_gather(windows.reshape(slots, -1), "req", axis=0, tiled=True)
    own_source = lax.dynamic_slice_in_dim(source, me * slots, slots)
    moved_windows = jnp.take(every_window, own_source, axis=0).reshape(windows.shape)

    x, xs = inputs_inner[0], inputs_state[0]
    taps = KERNEL - 1
    tail = jnp.concatenate([x[length - taps :], xs[length - taps :]], axis=1)
    position = lengths[0] - taps + jnp.arange(taps, dtype=jnp.int32) - rank * length
    inside = (position >= 0) & (position < length)
    clipped = jnp.clip(position, 0, length - 1)
    last = jnp.concatenate([jnp.take(x, clipped, axis=0), jnp.take(xs, clipped, axis=0)], axis=1)
    last = jnp.where(inside[:, None], last, jnp.zeros_like(last))
    edges = lax.all_gather(jnp.concatenate([tail, last], axis=0), "seq")
    head = lax.all_gather(moved_windows[0], "seq")
    head_inner = jnp.moveaxis(head[:, :, :own_width], 0, 1).reshape(taps, -1)
    head_outer = jnp.moveaxis(head[:, :, own_width:], 0, 1).reshape(taps, -1)
    before = lax.dynamic_index_in_dim(edges[:, :taps], lax.rem(rank + chain - 1, chain), 0, keepdims=False)
    window = jnp.where(rank == 0, jnp.concatenate([head_inner, head_outer], axis=1), before)
    window = jnp.pad(window.astype(jnp.float32), ((HALO - taps, 0), (0, 0)))
    kept = jnp.sum(edges[:, taps:].astype(jnp.float32), axis=0).astype(jnp.bfloat16)
    outer_own = state_window.shape[2]
    kept_inner = lax.dynamic_slice_in_dim(kept, rank * own_width, own_width, 1)
    kept_outer = lax.dynamic_slice_in_dim(kept, inner + rank * outer_own, outer_own, 1)
    new_inner = jnp.concatenate([kept_inner[None], moved_windows[1:, :, :own_width]], axis=0)
    new_outer = jnp.concatenate([kept_outer[None], moved_windows[1:, :, own_width:]], axis=0)

    valid_count = (lengths - rank * length).astype(jnp.int32)
    skip_row = jnp.repeat(skip_weight, HEAD_DIM)[None]
    part, end, ecum, read = mix(
        valid_count, x, xs, window, conv_weight, conv_bias, step_raw[0], step_bias, decay_log, skip_row
    )
    heads = decay_log.shape[0]
    ends = lax.all_gather(end, "seq")
    decays = lax.all_gather(ecum[length - 1, :heads], "seq")

    index = jnp.arange(chain)
    between = (index[None, :, None] > index[:, None, None]) & (index[None, :, None] < rank)
    coef = jnp.prod(jnp.where(between, decays[None], 1.0), axis=1) * (index[:, None] < rank)
    prior_decay = jnp.prod(jnp.where(index[:, None] < rank, decays, 1.0), axis=0)
    coef = jnp.concatenate([coef, prior_decay[None]], axis=0)
    coef_row = jnp.repeat(coef, HEAD_DIM, axis=1)
    after = index[None, :, None] > index[:, None, None]
    suffix = jnp.prod(jnp.where(after, decays[None], 1.0), axis=1)
    suffix = jnp.concatenate([suffix, jnp.prod(decays, axis=0)[None]], axis=0)
    suffix_own = jnp.repeat(lax.dynamic_slice_in_dim(suffix, rank * heads_own, heads_own, 1), HEAD_DIM, axis=1)

    send_first, send_rest = route(source, got, peers, slots)
    initial_own = exchange(send_first).reshape(rows, -1)
    rest = exchange(send_rest)
    initial = lax.all_gather(initial_own, "seq", axis=0, tiled=True)
    out = finish(valid_count, part, gate_rows[0], read, ecum, ends, coef_row, initial, norm_weight[None])

    ends_own = lax.dynamic_slice_in_dim(ends, rank * own_width, own_width, 2).astype(jnp.float32)
    final = jnp.sum(ends_own * suffix_own[:chain, None, :], axis=0).T
    final = final + suffix_own[chain][:, None] * initial_own.astype(jnp.float32)
    new_states = place(final[None], rest).reshape(pool_states.shape)
    return (new_states, new_inner, new_outer, out[None])


def solution(mesh):
    return jax.shard_map(
        on_device,
        mesh=mesh,
        in_specs=(
            P("req", "seq", None, None), P("req", None, "seq"), P("req", None, "seq"), P("req", None), P("req"),
            P("req", "seq", None), P("req", "seq", None), P("req", "seq", None), P("req", "seq", None), P("req"),
            P(), P(), P(), P(), P(), P(),
        ),
        out_specs=(
            P("req", "seq", None, None), P("req", None, "seq"), P("req", None, "seq"), P("req", "seq", None),
        ),
        check_vma=False,
    )
```

```python
import functools

import jax
import jax.numpy as jnp
from jax import lax
from jax.experimental import pallas as pl
from jax.experimental.pallas import tpu as pltpu
from jax.sharding import PartitionSpec as P

HEAD_DIM = 64
STATE_DIM = 128
KERNEL = 4
BLOCK_LEN = 256
EPSILON = 1e-05
LANES = 128
HALO = 8
LOG2E = 1.4426950408889634
GROUP = 2 * LANES


def half_silu(v):
    return (0.5 * v) * (1.0 + jnp.tanh(0.5 * v))


def conv_rows(ext_ref, weight_ref, bias_ref, start, count):
    total = bias_ref[...] + weight_ref[KERNEL - 1 : KERNEL, :] * ext_ref[pl.ds(start + HALO, count), :]
    for k in range(KERNEL - 1):
        total = total + weight_ref[k : k + 1, :] * ext_ref[pl.ds(start + HALO - KERNEL + 1 + k, count), :]
    return half_silu(total).astype(jnp.bfloat16)


def mix_kernel(
    nv_ref, x_ref, win_ref, cw_ref, cb_ref, skip_ref, xs_ref, wins_ref, cws_ref, cbs_ref, step_ref, sbias_ref, dlog_ref,
    part_ref, end_ref, ecum_ref, read_ref,
    ext, val, a_s, te_s, brow, write_t, score,
):
    g = pl.program_id(0)
    length = x_ref.shape[0]
    blocks = length // BLOCK_LEN
    half = BLOCK_LEN // 2

    @pl.when(g == 0)
    def _():
        ext[0:HALO, :] = wins_ref[...].astype(jnp.float32)
        ext[HALO : HALO + length, :] = xs_ref[...].astype(jnp.float32)
        ys = conv_rows(ext, cws_ref, cbs_ref, 0, length)
        write, read = ys[:, :STATE_DIM], ys[:, STATE_DIM:]
        read_ref[...] = read
        write_t[...] = write.astype(jnp.float32).T.astype(jnp.bfloat16)
        rows = lax.broadcasted_iota(jnp.int32, (length, LANES), 0)
        raw = step_ref[...] + sbias_ref[...]
        soft = jnp.maximum(raw, 0.0) + jnp.log1p(jnp.exp(-jnp.abs(raw)))
        dt = jnp.where(rows < nv_ref[0], soft, 0.0)
        rate = (dt * LOG2E) * (-jnp.exp(dlog_ref[...]))
        r = lax.broadcasted_iota(jnp.int32, (BLOCK_LEN, BLOCK_LEN), 0)
        c = lax.broadcasted_iota(jnp.int32, (BLOCK_LEN, BLOCK_LEN), 1)
        tri = (r >= c).astype(jnp.float32)
        before = jnp.zeros((1, LANES), jnp.float32)
        for blk in range(blocks):
            s = slice(blk * BLOCK_LEN, (blk + 1) * BLOCK_LEN)
            cum = jnp.dot(tri, rate[s], precision=lax.Precision.HIGHEST, preferred_element_type=jnp.float32)
            b = jnp.where(dt[s] > 0.0, cum - jnp.log2(dt[s]), 1e30)
            a_s[s, :] = cum
            last = cum[BLOCK_LEN - 1 : BLOCK_LEN, :]
            te_s[s, :] = jnp.exp2(last - b)
            brow[:, s] = b.T
            ecum_ref[s, :] = jnp.exp2(cum + before)
            before = before + last
            sc = lax.dot_general(read[s], write[s], (((1,), (1,)), ((), ())), preferred_element_type=jnp.float32)
            score[blk] = jnp.where(r >= c, sc, 0.0)

    ext[0:HALO, :] = win_ref[...].astype(jnp.float32)
    ext[HALO : HALO + length, :] = x_ref[...].astype(jnp.float32)
    rows_at_once = 64
    for i in range(length // rows_at_once):
        val[i * rows_at_once : (i + 1) * rows_at_once, :] = conv_rows(ext, cw_ref, cb_ref, i * rows_at_once, rows_at_once)

    heads_step = GROUP // HEAD_DIM
    turn = lax.rem(LANES - heads_step * g, LANES)
    a_all = pltpu.roll(a_s[...], turn, axis=1)
    te_all = pltpu.roll(te_s[...], turn, axis=1)
    low = lax.broadcasted_iota(jnp.int32, (1, LANES), 1) < HEAD_DIM

    for pair in range(GROUP // LANES):
        cols = slice(pair * LANES, (pair + 1) * LANES)
        skip = skip_ref[:, cols]
        before = None
        for blk in range(blocks):
            s = slice(blk * BLOCK_LEN, (blk + 1) * BLOCK_LEN)
            v = val[s, cols]
            vf = v.astype(jnp.float32)
            masked = [jnp.where(low, vf, 0.0).astype(jnp.bfloat16), jnp.where(low, 0.0, vf).astype(jnp.bfloat16)]
            tops, bottoms = [], []
            for j in range(2):
                h = 2 * pair + j
                a = a_all[s, h : h + 1]
                b = brow[pl.ds(heads_step * g + h, 1), s]
                top = jnp.exp2(jnp.minimum(a[:half] - b[:, :half], 126.0)) * score[blk, :half, :half]
                bot = jnp.exp2(jnp.minimum(a[half:] - b, 126.0)) * score[blk, half:, :]
                tops.append(top.astype(jnp.bfloat16))
                bottoms.append(bot.astype(jnp.bfloat16))
            intra_top = jnp.dot(
                jnp.concatenate(tops, axis=1), jnp.concatenate([m[:half] for m in masked], axis=0), preferred_element_type=jnp.float32
            )
            intra_bot = jnp.dot(
                jnp.concatenate(bottoms, axis=1), jnp.concatenate(masked, axis=0), preferred_element_type=jnp.float32
            )
            out = jnp.concatenate([intra_top, intra_bot], axis=0) + skip * vf
            h = 2 * pair
            te = jnp.where(low, te_all[s, h : h + 1], te_all[s, h + 1 : h + 2])
            state = jnp.dot(write_t[:, s], (te * vf).astype(jnp.bfloat16), preferred_element_type=jnp.float32)
            if blk > 0:
                e = jnp.exp2(jnp.where(low, a_all[s, h : h + 1], a_all[s, h + 1 : h + 2]))
                out = out + e * jnp.dot(read_ref[s, :], before.astype(jnp.bfloat16), preferred_element_type=jnp.float32)
                state = state + e[BLOCK_LEN - 1 : BLOCK_LEN, :] * before
            before = state
            part_ref[s, cols] = out.astype(jnp.bfloat16)
        end_ref[:, cols] = before.astype(jnp.bfloat16)


def mix(nv, x, xs, window, conv_weight, conv_bias, step_raw, step_bias, decay_log, skip_row):
    length, inner = x.shape
    pad = LANES - step_raw.shape[1]
    step = jnp.pad(step_raw.astype(jnp.float32), ((0, 0), (0, pad)))
    sbias = jnp.pad(step_bias, (0, pad))[None]
    dlog = jnp.pad(decay_log, (0, pad))[None]
    xs_width = xs.shape[1]
    beyond = inner // xs_width
    state_column = lambda rows: pl.BlockSpec((rows, xs_width), lambda i, nv: (0, beyond))
    fixed = lambda shape: pl.BlockSpec(shape, lambda i, nv: (0,) * len(shape))
    column = lambda rows: pl.BlockSpec((rows, GROUP), lambda i, nv: (0, i))
    blocks = length // BLOCK_LEN
    heads = inner // HEAD_DIM
    return pl.pallas_call(
        mix_kernel,
        grid_spec=pltpu.PrefetchScalarGridSpec(
            num_scalar_prefetch=1,
            grid=(inner // GROUP,),
            in_specs=[
                column(length), column(HALO), column(KERNEL), column(1), column(1),
                fixed((length, xs_width)), state_column(HALO), state_column(KERNEL), state_column(1),
                fixed((length, LANES)), fixed((1, LANES)), fixed((1, LANES)),
            ],
            out_specs=[column(length), column(STATE_DIM), fixed((length, LANES)), fixed((length, STATE_DIM))],
            scratch_shapes=[
                pltpu.VMEM((length + HALO, GROUP), jnp.float32),
                pltpu.VMEM((length, GROUP), jnp.bfloat16),
                pltpu.VMEM((length, LANES), jnp.float32),
                pltpu.VMEM((length, LANES), jnp.float32),
                pltpu.VMEM((LANES, length), jnp.float32),
                pltpu.VMEM((STATE_DIM, length), jnp.bfloat16),
                pltpu.VMEM((blocks, BLOCK_LEN, BLOCK_LEN), jnp.float32),
            ],
        ),
        out_shape=[
            jax.ShapeDtypeStruct((length, inner), jnp.bfloat16),
            jax.ShapeDtypeStruct((STATE_DIM, inner), jnp.bfloat16),
            jax.ShapeDtypeStruct((length, LANES), jnp.float32),
            jax.ShapeDtypeStruct((length, STATE_DIM), jnp.bfloat16),
        ],
        compiler_params=pltpu.CompilerParams(dimension_semantics=("arbitrary",)),
        cost_estimate=pl.CostEstimate(
            flops=2 * blocks * heads * BLOCK_LEN * BLOCK_LEN * LANES * 8,
            bytes_accessed=4 * length * inner, transcendentals=blocks * heads * BLOCK_LEN * BLOCK_LEN,
        ),
        name="mix",
    )(
        nv, x, window, conv_weight, conv_bias[None], skip_row, xs, window, conv_weight, conv_bias[None], step, sbias, dlog,
    )


CHUNK = 256


def finish_kernel(
    nv_ref, part_ref, gate_ref, read_ref, ecum_ref, coef_ref, init_ref, norm_ref, *refs
):
    out_ref, prior, spread, gated = refs[-4:]
    ends_refs = refs[:-4]
    step = pl.program_id(0)
    tile, inner = part_ref.shape
    links = len(ends_refs)
    chain = init_ref.shape[0]
    own_width = init_ref.shape[1]
    heads = inner // HEAD_DIM

    @pl.when(step == 0)
    def _():
        def fill(i, carry):
            cols = pl.ds(pl.multiple_of(i * CHUNK, CHUNK), CHUNK)
            total = coef_ref[0:1, cols] * ends_refs[0][:, cols].astype(jnp.float32)
            for j in range(1, links):
                total = total + coef_ref[j : j + 1, cols] * ends_refs[j][:, cols].astype(jnp.float32)
            prior[:, cols] = total.astype(jnp.bfloat16)
            k = lax.broadcasted_iota(jnp.int32, (LANES, CHUNK), 0)
            c = lax.broadcasted_iota(jnp.int32, (LANES, CHUNK), 1)
            owner = i * (CHUNK // HEAD_DIM) + c // HEAD_DIM
            spread[:, cols] = jnp.where((k == owner) | (k == owner + heads), 1.0, 0.0).astype(jnp.bfloat16)
            return carry

        lax.fori_loop(0, inner // CHUNK, fill, 0)

    read = read_ref[...]
    ecum = ecum_ref[...]
    first = ecum.astype(jnp.bfloat16).astype(jnp.float32)
    lane = lax.broadcasted_iota(jnp.int32, (tile, LANES), 1)
    both = jnp.where(lane < heads, first, pltpu.roll(ecum - first, heads, axis=1)).astype(jnp.bfloat16)
    rows = lax.broadcasted_iota(jnp.int32, (tile, 1), 0) + step * tile
    valid = (rows < nv_ref[0]).astype(jnp.float32)

    def gate_chunk(i, squares):
        cols = pl.ds(pl.multiple_of(i * CHUNK, CHUNK), CHUNK)
        z = jnp.dot(read, prior[:, cols], preferred_element_type=jnp.float32)
        chunks = own_width // CHUNK
        turned = lax.rem(nv_ref[1] + chain - i // chunks, chain)
        own = init_ref[turned, pl.ds(pl.multiple_of(lax.rem(i, chunks) * CHUNK, CHUNK), CHUNK), :]
        zi = lax.dot_general(read, own, (((1,), (1,)), ((), ())), preferred_element_type=jnp.float32)
        e = jnp.dot(both, spread[:, cols], preferred_element_type=jnp.float32)
        z = z + coef_ref[links : links + 1, cols] * zi
        y = (part_ref[:, cols].astype(jnp.float32) + e * z) * valid
        y = y.astype(jnp.bfloat16).astype(jnp.float32)
        out = y * half_silu(gate_ref[:, cols].astype(jnp.float32))
        gated[:, cols] = out
        square = out * out
        for k in range(CHUNK // LANES):
            squares = squares + square[:, k * LANES : (k + 1) * LANES]
        return squares

    squares = lax.fori_loop(0, inner // CHUNK, gate_chunk, jnp.zeros((tile, LANES), jnp.float32))
    scale = lax.rsqrt(jnp.sum(squares, axis=1, keepdims=True) * (1.0 / inner) + EPSILON)

    def scale_chunk(i, carry):
        cols = pl.ds(pl.multiple_of(i * CHUNK, CHUNK), CHUNK)
        out_ref[:, cols] = (gated[:, cols] * scale * norm_ref[:, cols]).astype(jnp.bfloat16)
        return carry

    lax.fori_loop(0, inner // CHUNK, scale_chunk, 0)


def finish(nv, part, gate, read, ecum, ends, coef, initial, norm):
    length, inner = part.shape
    tile = min(128, length)
    fixed = lambda shape: pl.BlockSpec(shape, lambda i, nv: (0,) * len(shape))
    row = lambda width: pl.BlockSpec((tile, width), lambda i, nv: (i, 0))
    return pl.pallas_call(
        finish_kernel,
        grid_spec=pltpu.PrefetchScalarGridSpec(
            num_scalar_prefetch=1,
            grid=(length // tile,),
            in_specs=[
                row(inner), row(inner), row(STATE_DIM), row(LANES),
                fixed(coef.shape), fixed(initial.shape), fixed((1, inner)), *[fixed(e.shape) for e in ends],
            ],
            out_specs=row(inner),
            scratch_shapes=[
                pltpu.VMEM((STATE_DIM, inner), jnp.bfloat16),
                pltpu.VMEM((LANES, inner), jnp.bfloat16),
                pltpu.VMEM((tile, inner), jnp.float32),
            ],
        ),
        out_shape=jax.ShapeDtypeStruct((length, inner), jnp.bfloat16),
        compiler_params=pltpu.CompilerParams(dimension_semantics=("arbitrary",)),
        cost_estimate=pl.CostEstimate(
            flops=40 * length * inner * STATE_DIM // 8, bytes_accessed=6 * length * inner, transcendentals=length * inner
        ),
        name="finish",
    )(nv, part, gate, read, ecum, coef, initial, norm, *ends)


def pack_kernel(keep_ref, state_ref, out_ref, held, packed, in_sem, out_sem):
    peers, slots, rows, _ = out_ref.shape

    def load(j):
        return pltpu.make_async_copy(state_ref.at[j], held.at[j], in_sem.at[j])

    def store(j):
        return pltpu.make_async_copy(packed.at[j], out_ref.at[:, j], out_sem.at[j])

    def first(j, carry):
        load(j).start()
        return carry

    def second(j, carry):
        load(j).wait()
        keep = keep_ref[j].astype(jnp.float32)
        for i in range(peers):
            packed[j, i] = (held[j, i * rows : (i + 1) * rows] * keep).astype(packed.dtype)
        store(j).start()
        return carry

    def third(j, carry):
        store(j).wait()
        return carry

    lax.fori_loop(0, slots, first, 0)
    lax.fori_loop(0, slots, second, 0)
    lax.fori_loop(0, slots, third, 0)


def pack_pieces(states, keep, peers):
    slots, rows, lanes = states.shape
    piece = rows // peers
    return pl.pallas_call(
        pack_kernel,
        in_specs=[pl.BlockSpec(memory_space=pltpu.SMEM), pl.BlockSpec(memory_space=pl.ANY)],
        out_specs=pl.BlockSpec(memory_space=pl.ANY),
        out_shape=jax.ShapeDtypeStruct((peers, slots, piece, lanes), jnp.bfloat16),
        scratch_shapes=[
            pltpu.VMEM((slots, rows, lanes), jnp.float32),
            pltpu.VMEM((slots, peers, piece, lanes), jnp.bfloat16),
            pltpu.SemaphoreType.DMA((slots,)),
            pltpu.SemaphoreType.DMA((slots,)),
        ],
        cost_estimate=pl.CostEstimate(flops=20 * slots * rows * lanes, bytes_accessed=6 * slots * rows * lanes, transcendentals=0),
        name="pack",
    )(keep, states)


def route_kernel(low, high, slots, source_ref, got_ref, out_ref, stage, in_sem, out_sem):
    peers = out_ref.shape[0]

    def one_peer(d, carry):
        for k in range(low, high):
            pltpu.make_async_copy(got_ref.at[source_ref[d * slots + k]], stage.at[d, k - low], in_sem).start()
        return carry

    lax.fori_loop(0, peers, one_peer, 0)
    pltpu.make_async_copy(out_ref, stage, in_sem).wait()
    copy = pltpu.make_async_copy(stage, out_ref, out_sem)
    copy.start()
    copy.wait()


def route(source, got, peers, low, high):
    count, rows, lanes = got.shape
    shape = (peers, high - low, rows, lanes)
    return pl.pallas_call(
        functools.partial(route_kernel, low, high, count // peers),
        in_specs=[pl.BlockSpec(memory_space=pltpu.SMEM), pl.BlockSpec(memory_space=pl.ANY)],
        out_specs=pl.BlockSpec(memory_space=pl.ANY),
        out_shape=jax.ShapeDtypeStruct(shape, got.dtype),
        scratch_shapes=[pltpu.VMEM(shape, got.dtype), pltpu.SemaphoreType.DMA, pltpu.SemaphoreType.DMA],
        cost_estimate=pl.CostEstimate(flops=10 * count * rows * lanes, bytes_accessed=4 * count * rows * lanes, transcendentals=0),
        name="route",
    )(source, got)


def place_kernel(offset, begin, count, got_ref, *refs):
    out_ref, held, wide, in_sem, out_sem = refs[-5:]
    peers, _, rows, _ = got_ref.shape

    def load(j):
        return pltpu.make_async_copy(got_ref.at[:, begin + j], held.at[j], in_sem.at[j])

    def store(j):
        return pltpu.make_async_copy(wide.at[j], out_ref.at[offset + j], out_sem.at[j])

    def first(j, carry):
        load(j).start()
        return carry

    def second(j, carry):
        load(j).wait()
        for i in range(peers):
            wide[j, i * rows : (i + 1) * rows] = held[j, i].astype(wide.dtype)
        store(j).start()
        return carry

    def third(j, carry):
        store(j).wait()
        return carry

    lax.fori_loop(0, count, first, 0)
    if begin > 0:
        final_ref, whole_ref, initial_ref = refs[:3]
        for i in range(0, final_ref.shape[1], LANES):
            own = slice(i, i + LANES)
            moved = initial_ref[own, :].astype(jnp.float32).T
            wide[count, own, :] = (final_ref[:, own] + whole_ref[:, own] * moved).T
        copy = pltpu.make_async_copy(wide.at[count], out_ref.at[0], out_sem.at[count])
        copy.start()
    lax.fori_loop(0, count, second, 0)
    lax.fori_loop(0, count, third, 0)
    if begin > 0:
        copy.wait()


def place(got, offset, begin, slots, final=None, placed=None):
    peers, total, rows, lanes = got.shape
    count = total - begin
    whole = pl.BlockSpec(memory_space=pl.ANY)
    operands, specs, alias = [got], [whole], {}
    if final is not None:
        operands += list(final)
        specs += [pl.BlockSpec(memory_space=pltpu.VMEM)] * len(final)
    if placed is not None:
        operands.append(placed)
        specs.append(whole)
        alias = {1: 0}
    return pl.pallas_call(
        functools.partial(place_kernel, offset, begin, count),
        in_specs=specs,
        out_specs=whole,
        out_shape=jax.ShapeDtypeStruct((slots, peers * rows, lanes), jnp.float32),
        scratch_shapes=[
            pltpu.VMEM((count, peers, rows, lanes), got.dtype),
            pltpu.VMEM((count + 1, peers * rows, lanes), jnp.float32),
            pltpu.SemaphoreType.DMA((count,)),
            pltpu.SemaphoreType.DMA((count + 1,)),
        ],
        input_output_aliases=alias,
        cost_estimate=pl.CostEstimate(
            flops=20 * count * peers * rows * lanes, bytes_accessed=6 * count * peers * rows * lanes, transcendentals=0
        ),
        name="place",
    )(*operands)


def letters_kernel(capacity, plan_ref, mask_ref, inner_ref, outer_ref, plan_row_ref, out_ref, table, count, wide_inner, wide_outer):
    taps, slots, inner = inner_ref.shape
    outer = outer_ref.shape[2]
    peers, rows, width = out_ref.shape
    wide_inner[...] = inner_ref[...].astype(jnp.float32)
    wide_outer[...] = outer_ref[...].astype(jnp.float32)

    def clear(d, carry):
        count[d] = 0
        for r in range(capacity):
            table[d * capacity + r] = -1
        return carry

    def enter(j, carry):
        d = plan_ref[0, j]
        table[d * capacity + count[d]] = jnp.where(mask_ref[j] != 0, j, -1)
        count[d] = count[d] + 1
        return carry

    lax.fori_loop(0, peers, clear, 0)
    lax.fori_loop(0, slots, enter, 0)

    def fill(d, carry):
        pieces = []
        for r in range(capacity):
            j = table[d * capacity + r]
            at = jnp.maximum(j, 0)
            for t in range(taps):
                row = jnp.concatenate(
                    [wide_inner[t, pl.ds(at, 1), :], wide_outer[t, pl.ds(at, 1), :], jnp.zeros((1, width - inner - outer), jnp.float32)],
                    axis=1,
                )
                pieces.append(jnp.where(j >= 0, row, 0.0))
        pieces.append(plan_row_ref[...])
        left = rows - taps * capacity - 1
        if left:
            pieces.append(jnp.zeros((left, width), jnp.float32))
        out_ref[d] = jnp.concatenate(pieces, axis=0).astype(out_ref.dtype)
        return carry

    lax.fori_loop(0, peers, fill, 0)


def letters(plan, mask, inner_window, outer_window, peers, capacity):
    slots, taps, inner = inner_window.shape
    outer = outer_window.shape[2]
    width = inner + outer
    width += -width % LANES
    rows = taps * capacity + 1
    rows += -rows % 16
    plan_row = jnp.concatenate([plan[:, 0], plan[:, 1], mask]).astype(jnp.float32)[None]
    plan_row = jnp.pad(plan_row, ((0, 0), (0, width - 3 * slots)))
    smem, vmem = pl.BlockSpec(memory_space=pltpu.SMEM), pl.BlockSpec(memory_space=pltpu.VMEM)
    return pl.pallas_call(
        functools.partial(letters_kernel, capacity),
        in_specs=[smem, smem, vmem, vmem, vmem],
        out_specs=vmem,
        out_shape=jax.ShapeDtypeStruct((peers, rows, width), jnp.bfloat16),
        scratch_shapes=[
            pltpu.SMEM((peers * capacity,), jnp.int32),
            pltpu.SMEM((peers,), jnp.int32),
            pltpu.VMEM((taps, slots, inner), jnp.float32),
            pltpu.VMEM((taps, slots, outer), jnp.float32),
        ],
        cost_estimate=pl.CostEstimate(flops=100000, bytes_accessed=8 * slots * taps * width, transcendentals=0),
        name="letters",
    )(plan.T, mask, jnp.moveaxis(inner_window, 1, 0), jnp.moveaxis(outer_window, 1, 0), plan_row)


def sort_kernel(low, high, table_ref, got_ref, *refs):
    stage, in_sem, out_sem = refs[-3:]
    outs = refs[:-3]
    count = high - low

    def one(k, carry):
        for m in range(len(outs)):
            pltpu.make_async_copy(got_ref.at[table_ref[m, low + k]], stage.at[m, k], in_sem.at[m]).start()
        return carry

    lax.fori_loop(0, count, one, 0)
    copies = [pltpu.make_async_copy(stage.at[m], outs[m], out_sem.at[m]) for m in range(len(outs))]
    for m in range(len(outs)):
        pltpu.make_async_copy(outs[m], stage.at[m], in_sem.at[m]).wait()
        copies[m].start()
    for copy in copies:
        copy.wait()


def sort_pieces(table, got, low, high):
    parts = table.shape[0]
    rows, lanes = got.shape[1:]
    shape = (high - low, rows, lanes)
    smem, whole = pl.BlockSpec(memory_space=pltpu.SMEM), pl.BlockSpec(memory_space=pl.ANY)
    return pl.pallas_call(
        functools.partial(sort_kernel, low, high),
        in_specs=[smem, whole],
        out_specs=[whole] * parts,
        out_shape=[jax.ShapeDtypeStruct(shape, jnp.bfloat16)] * parts,
        scratch_shapes=[pltpu.VMEM((parts,) + shape, jnp.bfloat16), pltpu.SemaphoreType.DMA((parts,)), pltpu.SemaphoreType.DMA((parts,))],
        cost_estimate=pl.CostEstimate(flops=10 * parts * high * rows * lanes, bytes_accessed=4 * parts * high * rows * lanes, transcendentals=0),
        name="sort",
    )(table, got)


def tables_kernel(peers, parts, slots, capacity, place_ref, plan_ref, near_ref, far_ref, info_ref, box_ref, need_ref, inverse):
    me, side, seat = place_ref[0], place_ref[1], place_ref[2]

    def one_source(r, carry):
        def one_slot(j, count):
            d, k = plan_ref[r, j], plan_ref[r, slots + j]
            inverse[d * slots + k] = (r * slots + j) * 2 + plan_ref[r, 2 * slots + j]

            @pl.when(d == me)
            def _():
                box_ref[k] = r * capacity + count

            return count + (d == me).astype(jnp.int32)

        lax.fori_loop(0, slots, one_slot, 0)
        return carry

    def clear(k, carry):
        for m in range(parts):
            near_ref[m, k] = 0
            far_ref[m, k] = 0
        return carry

    lax.fori_loop(0, peers, one_source, 0)
    lax.fori_loop(0, slots, clear, 0)

    def one_target(d, most):
        d_side = (d >= parts).astype(jnp.int32)
        m = lax.rem(d - d_side * parts + parts - seat, parts)

        def one_slot(k, count):
            code = inverse[d * slots + k]
            live = code % 2 == 1
            source = code // 2
            r = source // slots
            r_side = (r >= parts).astype(jnp.int32)
            held = source - r_side * (parts * slots)
            far = live & (r_side != d_side)
            at = jnp.where(k == 0, 0, count + 1)

            @pl.when(d == me)
            def _():
                info_ref[0, k] = jnp.where(live, jnp.where(far, 2, 1), 0)
                info_ref[1, k] = at
                info_ref[2, k] = seat

            @pl.when(live & (r_side == side) & (d_side == side))
            def _():
                near_ref[m, k] = held

            @pl.when(far & (r_side == side))
            def _():
                far_ref[m, at] = held

            return count + (far & (k > 0)).astype(jnp.int32)

        return jnp.maximum(most, lax.fori_loop(0, slots, one_slot, 0))

    need_ref[0] = lax.fori_loop(0, peers, one_target, 0)


def tables(place, plan, peers, parts, slots, capacity):
    smem = pl.BlockSpec(memory_space=pltpu.SMEM)
    ints = lambda *shape: jax.ShapeDtypeStruct(shape, jnp.int32)
    return pl.pallas_call(
        functools.partial(tables_kernel, peers, parts, slots, capacity),
        in_specs=[smem, smem],
        out_specs=[smem] * 5,
        out_shape=[ints(parts, slots), ints(parts, slots), ints(3, slots), ints(slots), ints(1)],
        scratch_shapes=[pltpu.SMEM((peers * slots,), jnp.int32)],
        cost_estimate=pl.CostEstimate(flops=1000000, bytes_accessed=4000, transcendentals=0),
        name="tables",
    )(place, plan)


def land_kernel(parts, info_ref, final_ref, whole_ref, initial_ref, *refs):
    near, far = refs[:parts], refs[parts : 2 * parts]
    out_ref, held, wide, in_sem, out_sem = refs[2 * parts :]
    rest, rows, _ = near[0].shape
    slots = rest + 1

    def each(k, act):
        kind, at = info_ref[0, k], info_ref[1, k]
        for m in range(parts):

            @pl.when(kind == 1)
            def _():
                act(pltpu.make_async_copy(near[m].at[k - 1], held.at[k, m], in_sem.at[k]))

            @pl.when(kind == 2)
            def _():
                act(pltpu.make_async_copy(far[m].at[at - 1], held.at[k, m], in_sem.at[k]))

    def store(k):
        return pltpu.make_async_copy(wide.at[k], out_ref.at[k], out_sem.at[k])

    def first(k, carry):
        each(k, lambda copy: copy.start())
        return carry

    def second(k, carry):
        each(k, lambda copy: copy.wait())
        kind = info_ref[0, k]
        for m in range(parts):
            begin = pl.multiple_of(lax.rem(info_ref[2, 1] + parts - m, parts) * rows, rows)
            wide[k, pl.ds(begin, rows)] = jnp.where(kind > 0, held[k, m].astype(wide.dtype), 0.0)
        store(k).start()
        return carry

    def third(k, carry):
        store(k).wait()
        return carry

    lax.fori_loop(1, slots, first, 0)
    for i in range(0, final_ref.shape[1], LANES):
        own = slice(i, i + LANES)
        moved = initial_ref[own, :].astype(jnp.float32).T
        wide[0, own, :] = (final_ref[:, own] + whole_ref[:, own] * moved).T
    store(0).start()
    lax.fori_loop(1, slots, second, 0)
    lax.fori_loop(0, slots, third, 0)


def land(info, final, whole_own, initial_own, near, far):
    parts = len(near)
    rest, rows, lanes = near[0].shape
    slots = rest + 1
    smem, vmem, whole = (pl.BlockSpec(memory_space=space) for space in (pltpu.SMEM, pltpu.VMEM, pl.ANY))
    return pl.pallas_call(
        functools.partial(land_kernel, parts),
        in_specs=[smem, vmem, vmem, vmem] + [whole] * (2 * parts),
        out_specs=whole,
        out_shape=jax.ShapeDtypeStruct((slots, parts * rows, lanes), jnp.float32),
        scratch_shapes=[
            pltpu.VMEM((slots, parts, rows, lanes), jnp.bfloat16),
            pltpu.VMEM((slots, parts * rows, lanes), jnp.float32),
            pltpu.SemaphoreType.DMA((slots,)),
            pltpu.SemaphoreType.DMA((slots,)),
        ],
        cost_estimate=pl.CostEstimate(
            flops=20 * slots * parts * rows * lanes, bytes_accessed=6 * slots * parts * rows * lanes, transcendentals=0
        ),
        name="land",
    )(info, final, whole_own, initial_own, *near, *far)


def exchange(source):
    return lax.all_to_all(source, "req", split_axis=0, concat_axis=0, tiled=True)


def shifts(value, axis):
    count = lax.axis_size(axis)
    return [value] + [lax.ppermute(value, axis, [(r, (r + k) % count) for r in range(count)]) for k in range(1, count)]


LIMITS = (6, 7, 8, 9)


def on_device(
    pool_states, inner_window, state_window, move_plan, active_mask, inputs_inner, inputs_state, gate_rows, step_raw,
    lengths, conv_weight, conv_bias, step_bias, decay_log, skip_weight, norm_weight,
):
    peers, me = lax.axis_size("req"), lax.axis_index("req")
    chain, rank = lax.axis_size("seq"), lax.axis_index("seq")
    slots, heads_own = pool_states.shape[:2]
    length, inner = inputs_inner.shape[1:]
    own_width = inner_window.shape[2]
    states = pool_states.reshape(slots, -1, pool_states.shape[-1])
    rows = states.shape[1]

    capacity = (2 * slots + peers - 1) // peers
    index = jnp.arange(slots, dtype=jnp.int32)
    sides = 2
    parts = peers // sides
    side, seat = me // parts, lax.rem(me, parts)
    with jax.named_scope("post"):
        every = exchange(letters(move_plan, active_mask, inner_window, state_window, peers, capacity))
    packed = pack_pieces(states, active_mask, parts)
    packed, every = lax.optimization_barrier((packed, every))
    with jax.named_scope("spread"):
        groups = [list(range(z * parts, (z + 1) * parts)) for z in range(sides)]
        got = lax.all_to_all(packed, "req", 0, 0, axis_index_groups=groups, tiled=True)
    got = got.reshape((parts * slots,) + got.shape[2:])

    def hop(value, across, by):
        pairs = [
            (z * parts + q, ((z + across) % sides) * parts + (q + by) % parts) for z in range(sides) for q in range(parts)
        ]
        return lax.ppermute(value, "req", pairs)

    taps = KERNEL - 1
    outer_own = state_window.shape[2]
    every_plan = every[:, taps * capacity, : 3 * slots].astype(jnp.int32)
    near_table, far_table, info, own_box, needed = tables(
        jnp.stack([me, side, seat]).astype(jnp.int32), every_plan, peers, parts, slots, capacity
    )
    came = every[:, : taps * capacity].reshape(peers * capacity, taps, -1)
    x, xs = inputs_inner[0], inputs_state[0]
    tail = jnp.concatenate([x[length - taps :], xs[length - taps :]], axis=1)
    head = lax.dynamic_index_in_dim(came, own_box[0], 0, keepdims=False)[:, : own_width + outer_own]
    with jax.named_scope("edge"):
        edges = lax.all_gather(jnp.concatenate([tail, head], axis=1), "seq")
    before = lax.dynamic_index_in_dim(edges, lax.rem(rank + chain - 1, chain), 0, keepdims=False)[:, : tail.shape[1]]
    head = edges[:, :, tail.shape[1] :]
    head_inner = jnp.moveaxis(head[:, :, :own_width], 0, 1).reshape(taps, -1)
    head_outer = jnp.moveaxis(head[:, :, own_width:], 0, 1).reshape(taps, -1)
    window = jnp.where(rank == 0, jnp.concatenate([head_inner, head_outer], axis=1), before)
    window = jnp.pad(window.astype(jnp.float32), ((HALO - taps, 0), (0, 0)))

    valid_count = (lengths - rank * length).astype(jnp.int32)
    skip_row = jnp.repeat(skip_weight, HEAD_DIM)[None]
    part, end, ecum, read = mix(
        valid_count, x, xs, window, conv_weight, conv_bias, step_raw[0], step_bias, decay_log, skip_row
    )
    heads = decay_log.shape[0]

    def arrive(limit, got, near_table, far_table, info, own_box, came, x, xs, part, end, ecum, read, gate):
        far_one = sort_pieces(far_table, got, 0, 1)
        far_first = [hop(far_one[m], 1, m) for m in range(parts)]
        near_one = sort_pieces(near_table, got, 0, 1)
        near_first = [near_one[0]] + [hop(near_one[m], 0, m) for m in range(1, parts)]
        far_all = sort_pieces(far_table, got, 1, limit + 1)
        far = [hop(far_all[m], 1, m) for m in range(parts)]
        near_all = sort_pieces(near_table, got, 1, slots)
        near = [near_all[0]] + [hop(near_all[m], 0, m) for m in range(1, parts)]
        decays = lax.all_gather(ecum[length - 1, :heads], "seq")
        index = jnp.arange(chain)
        ends, coef, total = [], [], end
        group = jnp.ones_like(decays[0])
        step = 1
        while step < chain:
            came_end = lax.ppermute(total, "seq", [(r, r ^ step) for r in range(chain)])
            upper = (rank // step) % 2
            base = (rank // (2 * step)) * (2 * step)
            second = (index >= base + step) & (index < base + 2 * step)
            first_half = (index >= base) & (index < base + step)
            second_decay = jnp.prod(jnp.where(second[:, None], decays, 1.0), axis=0)
            ends.append(came_end)
            coef.append(jnp.where(upper == 1, group, 0.0))
            group = jnp.where(upper == 1, group * jnp.prod(jnp.where(first_half[:, None], decays, 1.0), axis=0), group)
            row = jnp.repeat(second_decay, HEAD_DIM)[None]
            low, high = jnp.where(upper == 1, came_end, total), jnp.where(upper == 1, total, came_end)
            step *= 2
            if step < chain:
                total = (row * low.astype(jnp.float32) + high.astype(jnp.float32)).astype(jnp.bfloat16)
            else:
                own = lambda array: lax.dynamic_slice_in_dim(array, rank * own_width, own_width, 1)
                final = own(row) * own(low).astype(jnp.float32) + own(high).astype(jnp.float32)
        coef_row = jnp.repeat(jnp.stack(coef + [group]), HEAD_DIM, axis=1)
        whole = jnp.prod(decays, axis=0)
        whole_own = jnp.repeat(lax.dynamic_slice_in_dim(whole, rank * heads_own, heads_own), HEAD_DIM)[None]

        kind = info[0, 0]
        chosen = [
            jnp.where(kind == 1, near_first[m], jnp.where(kind == 2, far_first[m], jnp.zeros_like(far_first[m]))) for m in range(parts)
        ]
        initial_own = jnp.take(jnp.concatenate(chosen), lax.rem(seat + parts - jnp.arange(parts), parts), axis=0).reshape(rows, -1)
        initial = jnp.stack(shifts(initial_own, "seq"))
        out = finish(
            jnp.concatenate([valid_count, rank[None]]), part, gate, read, ecum, ends, coef_row, initial, norm_weight[None]
        )
        placed = land(info, final, whole_own, initial_own, near, far)
        position = lengths[0] - taps + jnp.arange(taps, dtype=jnp.int32) - rank * length
        inside = (position >= 0) & (position < length)
        clipped = jnp.clip(position, 0, length - 1)
        last = jnp.concatenate([jnp.take(x, clipped, axis=0), jnp.take(xs, clipped, axis=0)], axis=1)
        last = jnp.where(inside[:, None], last, jnp.zeros_like(last))
        kept = jnp.sum(lax.all_gather(last, "seq").astype(jnp.float32), axis=0).astype(jnp.bfloat16)
        kept_inner = lax.dynamic_slice_in_dim(kept, rank * own_width, own_width, 1)
        kept_outer = lax.dynamic_slice_in_dim(kept, inner + rank * outer_own, outer_own, 1)
        moved = jnp.take(came, own_box[1:], axis=0)
        new_inner = jnp.concatenate([kept_inner[None], moved[:, :, :own_width]], axis=0)
        new_outer = jnp.concatenate([kept_outer[None], moved[:, :, own_width : own_width + outer_own]], axis=0)
        return placed, out, new_inner, new_outer

    limits = sorted({min(slots - 1, limit) for limit in LIMITS} | {slots - 1})
    pick = sum((needed[0] > limit).astype(jnp.int32) for limit in limits[:-1])
    placed, out, new_inner, new_outer = lax.switch(
        pick, [functools.partial(arrive, limit) for limit in limits],
        got, near_table, far_table, info, own_box, came, x, xs, part, end, ecum, read, gate_rows[0],
    )
    return (placed.reshape(pool_states.shape), new_inner, new_outer, out[None])


def solution(mesh):
    return jax.shard_map(
        on_device,
        mesh=mesh,
        in_specs=(
            P("req", "seq", None, None), P("req", None, "seq"), P("req", None, "seq"), P("req", None), P("req"),
            P("req", "seq", None), P("req", "seq", None), P("req", "seq", None), P("req", "seq", None), P("req"),
            P(), P(), P(), P(), P(), P(),
        ),
        out_specs=(
            P("req", "seq", None, None), P("req", None, "seq"), P("req", None, "seq"), P("req", "seq", None),
        ),
        check_vma=False,
    )
```

```python
import functools

import jax
import jax.numpy as jnp
from jax import lax
from jax.experimental import pallas as pl
from jax.experimental.pallas import tpu as pltpu
from jax.sharding import PartitionSpec as P


HEAD_DIM = 64
STATE_DIM = 128
KERNEL = 4
BLOCK_LEN = 256
EPSILON = 1e-05
LANES = 128
HALO = 8
LOG2E = 1.4426950408889634
GROUP = 2 * LANES


def half_silu(v):
    return (0.5 * v) * (1.0 + jnp.tanh(0.5 * v))


def conv_rows(ext_ref, weight_ref, bias_ref, start, count):
    total = bias_ref[...] + weight_ref[KERNEL - 1 : KERNEL, :] * ext_ref[pl.ds(start + HALO, count), :]
    for k in range(KERNEL - 1):
        total = total + weight_ref[k : k + 1, :] * ext_ref[pl.ds(start + HALO - KERNEL + 1 + k, count), :]
    return half_silu(total).astype(jnp.bfloat16)


def mix_kernel(
    nv_ref, x_ref, win_ref, cw_ref, cb_ref, skip_ref, xs_ref, wins_ref, cws_ref, cbs_ref, step_ref, sbias_ref, dlog_ref,
    part_ref, end_ref, ecum_ref, read_ref,
    ext, val, a_s, te_s, brow, write_t, score,
):
    g = pl.program_id(0)
    length = x_ref.shape[0]
    blocks = length // BLOCK_LEN
    half = BLOCK_LEN // 2

    @pl.when(g == 0)
    def _():
        ext[0:HALO, :] = wins_ref[...].astype(jnp.float32)
        ext[HALO : HALO + length, :] = xs_ref[...].astype(jnp.float32)
        ys = conv_rows(ext, cws_ref, cbs_ref, 0, length)
        write, read = ys[:, :STATE_DIM], ys[:, STATE_DIM:]
        read_ref[...] = read
        write_t[...] = write.astype(jnp.float32).T.astype(jnp.bfloat16)
        rows = lax.broadcasted_iota(jnp.int32, (length, LANES), 0)
        raw = step_ref[...] + sbias_ref[...]
        soft = jnp.maximum(raw, 0.0) + jnp.log1p(jnp.exp(-jnp.abs(raw)))
        dt = jnp.where(rows < nv_ref[0], soft, 0.0)
        rate = (dt * LOG2E) * (-jnp.exp(dlog_ref[...]))
        r = lax.broadcasted_iota(jnp.int32, (BLOCK_LEN, BLOCK_LEN), 0)
        c = lax.broadcasted_iota(jnp.int32, (BLOCK_LEN, BLOCK_LEN), 1)
        tri = (r >= c).astype(jnp.float32)
        before = jnp.zeros((1, LANES), jnp.float32)
        for blk in range(blocks):
            s = slice(blk * BLOCK_LEN, (blk + 1) * BLOCK_LEN)
            cum = jnp.dot(tri, rate[s], precision=lax.Precision.HIGHEST, preferred_element_type=jnp.float32)
            b = jnp.where(dt[s] > 0.0, cum - jnp.log2(dt[s]), 1e30)
            a_s[s, :] = cum
            last = cum[BLOCK_LEN - 1 : BLOCK_LEN, :]
            te_s[s, :] = jnp.exp2(last - b)
            brow[:, s] = b.T
            ecum_ref[s, :] = jnp.exp2(cum + before)
            before = before + last
            sc = lax.dot_general(read[s], write[s], (((1,), (1,)), ((), ())), preferred_element_type=jnp.float32)
            score[blk] = jnp.where(r >= c, sc, 0.0)

    ext[0:HALO, :] = win_ref[...].astype(jnp.float32)
    ext[HALO : HALO + length, :] = x_ref[...].astype(jnp.float32)
    rows_at_once = 64
    for i in range(length // rows_at_once):
        val[i * rows_at_once : (i + 1) * rows_at_once, :] = conv_rows(ext, cw_ref, cb_ref, i * rows_at_once, rows_at_once)

    heads_step = GROUP // HEAD_DIM
    turn = lax.rem(LANES - heads_step * g, LANES)
    a_all = pltpu.roll(a_s[...], turn, axis=1)
    te_all = pltpu.roll(te_s[...], turn, axis=1)
    low = lax.broadcasted_iota(jnp.int32, (1, LANES), 1) < HEAD_DIM

    for pair in range(GROUP // LANES):
        cols = slice(pair * LANES, (pair + 1) * LANES)
        skip = skip_ref[:, cols]
        before = None
        for blk in range(blocks):
            s = slice(blk * BLOCK_LEN, (blk + 1) * BLOCK_LEN)
            v = val[s, cols]
            vf = v.astype(jnp.float32)
            masked = [jnp.where(low, vf, 0.0).astype(jnp.bfloat16), jnp.where(low, 0.0, vf).astype(jnp.bfloat16)]
            tops, bottoms = [], []
            for j in range(2):
                h = 2 * pair + j
                a = a_all[s, h : h + 1]
                b = brow[pl.ds(heads_step * g + h, 1), s]
                top = jnp.exp2(jnp.minimum(a[:half] - b[:, :half], 126.0)) * score[blk, :half, :half]
                bot = jnp.exp2(jnp.minimum(a[half:] - b, 126.0)) * score[blk, half:, :]
                tops.append(top.astype(jnp.bfloat16))
                bottoms.append(bot.astype(jnp.bfloat16))
            intra_top = jnp.dot(
                jnp.concatenate(tops, axis=1), jnp.concatenate([m[:half] for m in masked], axis=0), preferred_element_type=jnp.float32
            )
            intra_bot = jnp.dot(
                jnp.concatenate(bottoms, axis=1), jnp.concatenate(masked, axis=0), preferred_element_type=jnp.float32
            )
            out = jnp.concatenate([intra_top, intra_bot], axis=0) + skip * vf
            h = 2 * pair
            te = jnp.where(low, te_all[s, h : h + 1], te_all[s, h + 1 : h + 2])
            state = jnp.dot(write_t[:, s], (te * vf).astype(jnp.bfloat16), preferred_element_type=jnp.float32)
            if blk > 0:
                e = jnp.exp2(jnp.where(low, a_all[s, h : h + 1], a_all[s, h + 1 : h + 2]))
                out = out + e * jnp.dot(read_ref[s, :], before.astype(jnp.bfloat16), preferred_element_type=jnp.float32)
                state = state + e[BLOCK_LEN - 1 : BLOCK_LEN, :] * before
            before = state
            part_ref[s, cols] = out.astype(jnp.bfloat16)
        end_ref[:, cols] = before.astype(jnp.bfloat16)


def mix(nv, x, xs, window, conv_weight, conv_bias, step_raw, step_bias, decay_log, skip_row):
    length, inner = x.shape
    pad = LANES - step_raw.shape[1]
    step = jnp.pad(step_raw.astype(jnp.float32), ((0, 0), (0, pad)))
    sbias = jnp.pad(step_bias, (0, pad))[None]
    dlog = jnp.pad(decay_log, (0, pad))[None]
    xs_width = xs.shape[1]
    beyond = inner // xs_width
    state_column = lambda rows: pl.BlockSpec((rows, xs_width), lambda i, nv: (0, beyond))
    fixed = lambda shape: pl.BlockSpec(shape, lambda i, nv: (0,) * len(shape))
    column = lambda rows: pl.BlockSpec((rows, GROUP), lambda i, nv: (0, i))
    blocks = length // BLOCK_LEN
    heads = inner // HEAD_DIM
    return pl.pallas_call(
        mix_kernel,
        grid_spec=pltpu.PrefetchScalarGridSpec(
            num_scalar_prefetch=1,
            grid=(inner // GROUP,),
            in_specs=[
                column(length), column(HALO), column(KERNEL), column(1), column(1),
                fixed((length, xs_width)), state_column(HALO), state_column(KERNEL), state_column(1),
                fixed((length, LANES)), fixed((1, LANES)), fixed((1, LANES)),
            ],
            out_specs=[column(length), column(STATE_DIM), fixed((length, LANES)), fixed((length, STATE_DIM))],
            scratch_shapes=[
                pltpu.VMEM((length + HALO, GROUP), jnp.float32),
                pltpu.VMEM((length, GROUP), jnp.bfloat16),
                pltpu.VMEM((length, LANES), jnp.float32),
                pltpu.VMEM((length, LANES), jnp.float32),
                pltpu.VMEM((LANES, length), jnp.float32),
                pltpu.VMEM((STATE_DIM, length), jnp.bfloat16),
                pltpu.VMEM((blocks, BLOCK_LEN, BLOCK_LEN), jnp.float32),
            ],
        ),
        out_shape=[
            jax.ShapeDtypeStruct((length, inner), jnp.bfloat16),
            jax.ShapeDtypeStruct((STATE_DIM, inner), jnp.bfloat16),
            jax.ShapeDtypeStruct((length, LANES), jnp.float32),
            jax.ShapeDtypeStruct((length, STATE_DIM), jnp.bfloat16),
        ],
        compiler_params=pltpu.CompilerParams(dimension_semantics=("arbitrary",)),
        cost_estimate=pl.CostEstimate(
            flops=2 * blocks * heads * BLOCK_LEN * BLOCK_LEN * LANES * 8,
            bytes_accessed=4 * length * inner, transcendentals=blocks * heads * BLOCK_LEN * BLOCK_LEN,
        ),
        name="mix",
    )(
        nv, x, window, conv_weight, conv_bias[None], skip_row, xs, window, conv_weight, conv_bias[None], step, sbias, dlog,
    )


CHUNK = 256


def finish_kernel(
    nv_ref, part_ref, gate_ref, read_ref, ecum_ref, coef_ref, init_ref, norm_ref, *refs
):
    out_ref, token_ref, prior, spread, gated = refs[-5:]
    ends_refs = refs[:-5]
    token_ref[0] = 0
    step = pl.program_id(0)
    tile, inner = part_ref.shape
    links = len(ends_refs)
    own_width = init_ref.shape[1]
    heads = inner // HEAD_DIM

    @pl.when(step == 0)
    def _():
        def fill(i, carry):
            cols = pl.ds(pl.multiple_of(i * CHUNK, CHUNK), CHUNK)
            total = coef_ref[0:1, cols] * ends_refs[0][:, cols].astype(jnp.float32)
            for j in range(1, links):
                total = total + coef_ref[j : j + 1, cols] * ends_refs[j][:, cols].astype(jnp.float32)
            prior[:, cols] = total.astype(jnp.bfloat16)
            k = lax.broadcasted_iota(jnp.int32, (LANES, CHUNK), 0)
            c = lax.broadcasted_iota(jnp.int32, (LANES, CHUNK), 1)
            owner = i * (CHUNK // HEAD_DIM) + c // HEAD_DIM
            spread[:, cols] = jnp.where((k == owner) | (k == owner + heads), 1.0, 0.0).astype(jnp.bfloat16)
            return carry

        lax.fori_loop(0, inner // CHUNK, fill, 0)

    read = read_ref[...]
    ecum = ecum_ref[...]
    first = ecum.astype(jnp.bfloat16).astype(jnp.float32)
    lane = lax.broadcasted_iota(jnp.int32, (tile, LANES), 1)
    both = jnp.where(lane < heads, first, pltpu.roll(ecum - first, heads, axis=1)).astype(jnp.bfloat16)
    rows = lax.broadcasted_iota(jnp.int32, (tile, 1), 0) + step * tile
    valid = (rows < nv_ref[0]).astype(jnp.float32)

    def gate_chunk(i, squares):
        cols = pl.ds(pl.multiple_of(i * CHUNK, CHUNK), CHUNK)
        z = jnp.dot(read, prior[:, cols], preferred_element_type=jnp.float32)
        chunks = own_width // CHUNK
        turned = nv_ref[1] ^ (i // chunks)
        own = init_ref[turned, pl.ds(pl.multiple_of(lax.rem(i, chunks) * CHUNK, CHUNK), CHUNK), :]
        zi = lax.dot_general(read, own, (((1,), (1,)), ((), ())), preferred_element_type=jnp.float32)
        e = jnp.dot(both, spread[:, cols], preferred_element_type=jnp.float32)
        z = z + coef_ref[links : links + 1, cols] * zi
        y = (part_ref[:, cols].astype(jnp.float32) + e * z) * valid
        y = y.astype(jnp.bfloat16).astype(jnp.float32)
        out = y * half_silu(gate_ref[:, cols].astype(jnp.float32))
        gated[:, cols] = out
        square = out * out
        for k in range(CHUNK // LANES):
            squares = squares + square[:, k * LANES : (k + 1) * LANES]
        return squares

    squares = lax.fori_loop(0, inner // CHUNK, gate_chunk, jnp.zeros((tile, LANES), jnp.float32), unroll=2)
    scale = lax.rsqrt(jnp.sum(squares, axis=1, keepdims=True) * (1.0 / inner) + EPSILON)

    def scale_chunk(i, carry):
        cols = pl.ds(pl.multiple_of(i * CHUNK, CHUNK), CHUNK)
        out_ref[:, cols] = (gated[:, cols] * scale * norm_ref[:, cols]).astype(jnp.bfloat16)
        return carry

    lax.fori_loop(0, inner // CHUNK, scale_chunk, 0, unroll=2)


def finish(nv, part, gate, read, ecum, ends, coef, initial, norm):
    length, inner = part.shape
    tile = min(128, length)
    fixed = lambda shape: pl.BlockSpec(shape, lambda i, nv: (0,) * len(shape))
    row = lambda width: pl.BlockSpec((tile, width), lambda i, nv: (i, 0))
    return pl.pallas_call(
        finish_kernel,
        grid_spec=pltpu.PrefetchScalarGridSpec(
            num_scalar_prefetch=1,
            grid=(length // tile,),
            in_specs=[
                row(inner), row(inner), row(STATE_DIM), row(LANES),
                fixed(coef.shape), fixed(initial.shape), fixed((1, inner)), *[fixed(e.shape) for e in ends],
            ],
            out_specs=[row(inner), pl.BlockSpec(memory_space=pltpu.SMEM)],
            scratch_shapes=[
                pltpu.VMEM((STATE_DIM, inner), jnp.bfloat16),
                pltpu.VMEM((LANES, inner), jnp.bfloat16),
                pltpu.VMEM((tile, inner), jnp.float32),
            ],
        ),
        out_shape=[jax.ShapeDtypeStruct((length, inner), jnp.bfloat16), jax.ShapeDtypeStruct((1,), jnp.int32)],
        compiler_params=pltpu.CompilerParams(dimension_semantics=("arbitrary",)),
        cost_estimate=pl.CostEstimate(
            flops=40 * length * inner * STATE_DIM // 8, bytes_accessed=6 * length * inner, transcendentals=length * inner
        ),
        name="finish",
    )(nv, part, gate, read, ecum, coef, initial, norm, *ends)


def pack_kernel(keep_ref, state_ref, out_ref, held, packed, in_sem, out_sem):
    peers, slots, rows, _ = out_ref.shape

    def load(j):
        return pltpu.make_async_copy(state_ref.at[j], held.at[j], in_sem.at[j])

    def store(j):
        return pltpu.make_async_copy(packed.at[j], out_ref.at[:, j], out_sem.at[j])

    def first(j, carry):
        load(j).start()
        return carry

    def second(j, carry):
        load(j).wait()
        keep = keep_ref[j].astype(jnp.float32)
        for i in range(peers):
            packed[j, i] = (held[j, i * rows : (i + 1) * rows] * keep).astype(packed.dtype)
        store(j).start()
        return carry

    def third(j, carry):
        store(j).wait()
        return carry

    lax.fori_loop(0, slots, first, 0)
    lax.fori_loop(0, slots, second, 0)
    lax.fori_loop(0, slots, third, 0)


def pack_pieces(states, keep, peers):
    slots, rows, lanes = states.shape
    piece = rows // peers
    return pl.pallas_call(
        pack_kernel,
        in_specs=[pl.BlockSpec(memory_space=pltpu.SMEM), pl.BlockSpec(memory_space=pl.ANY)],
        out_specs=pl.BlockSpec(memory_space=pl.ANY),
        out_shape=jax.ShapeDtypeStruct((peers, slots, piece, lanes), jnp.bfloat16),
        scratch_shapes=[
            pltpu.VMEM((slots, rows, lanes), jnp.float32),
            pltpu.VMEM((slots, peers, piece, lanes), jnp.bfloat16),
            pltpu.SemaphoreType.DMA((slots,)),
            pltpu.SemaphoreType.DMA((slots,)),
        ],
        cost_estimate=pl.CostEstimate(flops=20 * slots * rows * lanes, bytes_accessed=6 * slots * rows * lanes, transcendentals=0),
        name="pack",
    )(keep, states)


def letters_kernel(capacity, plan_ref, mask_ref, inner_ref, outer_ref, plan_row_ref, out_ref, table, count, wide_inner, wide_outer):
    taps, slots, inner = inner_ref.shape
    outer = outer_ref.shape[2]
    peers, rows, width = out_ref.shape
    wide_inner[...] = inner_ref[...].astype(jnp.float32)
    wide_outer[...] = outer_ref[...].astype(jnp.float32)

    def clear(d, carry):
        count[d] = 0
        for r in range(capacity):
            table[d * capacity + r] = -1
        return carry

    def enter(j, carry):
        d = plan_ref[0, j]
        table[d * capacity + count[d]] = jnp.where(mask_ref[j] != 0, j, -1)
        count[d] = count[d] + 1
        return carry

    lax.fori_loop(0, peers, clear, 0)
    lax.fori_loop(0, slots, enter, 0)

    def fill(d, carry):
        pieces = []
        for r in range(capacity):
            j = table[d * capacity + r]
            at = jnp.maximum(j, 0)
            for t in range(taps):
                row = jnp.concatenate(
                    [wide_inner[t, pl.ds(at, 1), :], wide_outer[t, pl.ds(at, 1), :], jnp.zeros((1, width - inner - outer), jnp.float32)],
                    axis=1,
                )
                pieces.append(jnp.where(j >= 0, row, 0.0))
        pieces.append(plan_row_ref[...])
        left = rows - taps * capacity - 1
        if left:
            pieces.append(jnp.zeros((left, width), jnp.float32))
        out_ref[d] = jnp.concatenate(pieces, axis=0).astype(out_ref.dtype)
        return carry

    lax.fori_loop(0, peers, fill, 0)


def letters(plan, mask, inner_window, outer_window, peers, capacity):
    slots, taps, inner = inner_window.shape
    outer = outer_window.shape[2]
    width = inner + outer
    width += -width % LANES
    rows = taps * capacity + 1
    rows += -rows % 16
    plan_row = jnp.concatenate([plan[:, 0], plan[:, 1], mask]).astype(jnp.float32)[None]
    plan_row = jnp.pad(plan_row, ((0, 0), (0, width - 3 * slots)))
    smem, vmem = pl.BlockSpec(memory_space=pltpu.SMEM), pl.BlockSpec(memory_space=pltpu.VMEM)
    return pl.pallas_call(
        functools.partial(letters_kernel, capacity),
        in_specs=[smem, smem, vmem, vmem, vmem],
        out_specs=vmem,
        out_shape=jax.ShapeDtypeStruct((peers, rows, width), jnp.bfloat16),
        scratch_shapes=[
            pltpu.SMEM((peers * capacity,), jnp.int32),
            pltpu.SMEM((peers,), jnp.int32),
            pltpu.VMEM((taps, slots, inner), jnp.float32),
            pltpu.VMEM((taps, slots, outer), jnp.float32),
        ],
        cost_estimate=pl.CostEstimate(flops=100000, bytes_accessed=8 * slots * taps * width, transcendentals=0),
        name="letters",
    )(plan.T, mask, jnp.moveaxis(inner_window, 1, 0), jnp.moveaxis(outer_window, 1, 0), plan_row)


def sort_kernel(table_ref, got_ref, *refs):
    stage, in_sem, out_sem = refs[-3:]
    outs, token_ref = refs[:-4], refs[-4]
    parts, count = stage.shape[:2]
    token_ref[0] = 0

    def one(k, carry):
        for m in range(parts):
            pltpu.make_async_copy(got_ref.at[table_ref[m, k]], stage.at[m, k], in_sem.at[m]).start()
        return carry

    lax.fori_loop(0, count, one, 0)
    copies = [pltpu.make_async_copy(stage.at[m], outs[m], out_sem.at[m]) for m in range(parts)]
    for m in range(parts):
        pltpu.make_async_copy(got_ref.at[0:count], stage.at[m], in_sem.at[m]).wait()
        copies[m].start()
    for copy in copies:
        copy.wait()


def sort_pieces(table, got, count):
    parts = table.shape[0]
    rows, lanes = got.shape[1:]
    smem, whole = pl.BlockSpec(memory_space=pltpu.SMEM), pl.BlockSpec(memory_space=pl.ANY)
    *outs, token = pl.pallas_call(
        sort_kernel,
        in_specs=[smem, whole],
        out_specs=[whole] * parts + [smem],
        out_shape=[jax.ShapeDtypeStruct((count, rows, lanes), jnp.bfloat16)] * parts + [jax.ShapeDtypeStruct((1,), jnp.int32)],
        scratch_shapes=[
            pltpu.VMEM((parts, count, rows, lanes), jnp.bfloat16),
            pltpu.SemaphoreType.DMA((parts,)),
            pltpu.SemaphoreType.DMA((parts,)),
        ],
        cost_estimate=pl.CostEstimate(flops=10 * parts * count * rows * lanes, bytes_accessed=4 * parts * count * rows * lanes, transcendentals=0),
        name="sort",
    )(table, got)
    return outs, token[0]


def tables_kernel(peers, parts, slots, capacity, place_ref, plan_ref, near_ref, far_ref, first_ref, info_ref, box_ref, need_ref, inverse):
    me, side, seat = place_ref[0], place_ref[1], place_ref[2]

    def one_source(r, carry):
        def one_slot(j, count):
            d, k = plan_ref[r, j], plan_ref[r, slots + j]
            inverse[d * slots + k] = (r << 9) + (j << 1) + plan_ref[r, 2 * slots + j]

            @pl.when(d == me)
            def _():
                box_ref[k] = r * capacity + count

            return count + (d == me).astype(jnp.int32)

        lax.fori_loop(0, slots, one_slot, 0)
        return carry

    def clear(k, carry):
        for m in range(parts):
            near_ref[m, k] = 0
            far_ref[m, k] = 0
        return carry

    lax.fori_loop(0, peers, one_source, 0)
    lax.fori_loop(0, slots - 1, clear, 0)

    def one_target(d, most):
        d_side = (d >= parts).astype(jnp.int32)
        m = lax.rem(d - d_side * parts + parts - seat, parts)

        def one_slot(k, count):
            code = inverse[d * slots + k]
            live = (code & 1) == 1
            r = code >> 9
            r_side = (r >= parts).astype(jnp.int32)
            held = (r - r_side * parts) * slots + ((code >> 1) & 255)
            far = live & (r_side != d_side)

            @pl.when(d == me)
            def _():
                info_ref[0, k] = jnp.where(live, jnp.where(far, 2, 1), 0)
                info_ref[1, k] = count
                info_ref[2, k] = seat

            @pl.when(k == 0)
            def _():
                first_ref[0, d] = jnp.where(live & (r_side == side), held, 0)

            @pl.when(live & (k > 0) & (r_side == side) & (d_side == side))
            def _():
                near_ref[m, k - 1] = held

            @pl.when(far & (k > 0) & (r_side == side))
            def _():
                far_ref[m, count] = held

            return count + (far & (k > 0)).astype(jnp.int32)

        return jnp.maximum(most, lax.fori_loop(0, slots, one_slot, 0))

    need_ref[0] = lax.fori_loop(0, peers, one_target, 0)


def tables(place, plan, peers, parts, slots, capacity):
    smem = pl.BlockSpec(memory_space=pltpu.SMEM)
    ints = lambda *shape: jax.ShapeDtypeStruct(shape, jnp.int32)
    return pl.pallas_call(
        functools.partial(tables_kernel, peers, parts, slots, capacity),
        in_specs=[smem, smem],
        out_specs=[smem] * 6,
        out_shape=[ints(parts, slots - 1), ints(parts, slots - 1), ints(1, peers), ints(3, slots), ints(slots), ints(1)],
        scratch_shapes=[pltpu.SMEM((peers * slots,), jnp.int32)],
        cost_estimate=pl.CostEstimate(flops=1000000, bytes_accessed=4000, transcendentals=0),
        name="tables",
    )(place, plan)


def land_kernel(parts, info_ref, final_ref, whole_ref, initial_ref, *refs):
    near, far = refs[:parts], refs[parts : 2 * parts]
    out_ref, held, wide, in_sem, out_sem = refs[2 * parts :]
    rest, rows, _ = near[0].shape
    slots = rest + 1

    def each(k, act):
        kind, at = info_ref[0, k], info_ref[1, k]
        for m in range(parts):

            @pl.when(kind == 1)
            def _():
                act(pltpu.make_async_copy(near[m].at[k - 1], held.at[k, m], in_sem.at[k]))

            @pl.when(kind == 2)
            def _():
                act(pltpu.make_async_copy(far[m].at[at], held.at[k, m], in_sem.at[k]))

    def store(k):
        return pltpu.make_async_copy(wide.at[k], out_ref.at[k], out_sem.at[k])

    def first(k, carry):
        each(k, lambda copy: copy.start())
        return carry

    def second(k, carry):
        each(k, lambda copy: copy.wait())
        kind = info_ref[0, k]
        for m in range(parts):
            begin = pl.multiple_of(lax.rem(info_ref[2, 1] + parts - m, parts) * rows, rows)
            wide[k, pl.ds(begin, rows)] = jnp.where(kind > 0, held[k, m].astype(wide.dtype), 0.0)
        store(k).start()
        return carry

    def third(k, carry):
        store(k).wait()
        return carry

    lax.fori_loop(1, slots, first, 0)
    for i in range(0, final_ref.shape[1], LANES):
        own = slice(i, i + LANES)
        moved = initial_ref[own, :].astype(jnp.float32).T
        wide[0, own, :] = (final_ref[:, own] + whole_ref[:, own] * moved).T
    store(0).start()
    lax.fori_loop(1, slots, second, 0)
    lax.fori_loop(0, slots, third, 0)


def land(info, final, whole_own, initial_own, near, far):
    parts = len(near)
    rest, rows, lanes = near[0].shape
    slots = rest + 1
    smem, vmem, whole = (pl.BlockSpec(memory_space=space) for space in (pltpu.SMEM, pltpu.VMEM, pl.ANY))
    return pl.pallas_call(
        functools.partial(land_kernel, parts),
        in_specs=[smem, vmem, vmem, vmem] + [whole] * (2 * parts),
        out_specs=whole,
        out_shape=jax.ShapeDtypeStruct((slots, parts * rows, lanes), jnp.float32),
        scratch_shapes=[
            pltpu.VMEM((slots, parts, rows, lanes), jnp.bfloat16),
            pltpu.VMEM((slots, parts * rows, lanes), jnp.float32),
            pltpu.SemaphoreType.DMA((slots,)),
            pltpu.SemaphoreType.DMA((slots,)),
        ],
        cost_estimate=pl.CostEstimate(
            flops=20 * slots * parts * rows * lanes, bytes_accessed=6 * slots * parts * rows * lanes, transcendentals=0
        ),
        name="land",
    )(info, final, whole_own, initial_own, *near, *far)


def exchange(source):
    return lax.all_to_all(source, "req", split_axis=0, concat_axis=0, tiled=True)


def flip(value, axis, step):
    return lax.ppermute(value, axis, [(r, r ^ step) for r in range(lax.axis_size(axis))])


def by_mask(value, axis):
    held, step = {0: value}, lax.axis_size(axis) // 2
    while step:
        masks = sorted(held)
        came = flip(jnp.stack([held[m] for m in masks]) if len(masks) > 1 else held[masks[0]][None], axis, step)
        held.update({m ^ step: came[i] for i, m in enumerate(masks)})
        step //= 2
    return [held[m] for m in sorted(held)]


LIMITS = (7, 9)


def on_device(
    pool_states, inner_window, state_window, move_plan, active_mask, inputs_inner, inputs_state, gate_rows, step_raw,
    lengths, conv_weight, conv_bias, step_bias, decay_log, skip_weight, norm_weight,
):
    peers, me = lax.axis_size("req"), lax.axis_index("req")
    chain, rank = lax.axis_size("seq"), lax.axis_index("seq")
    slots, _ = pool_states.shape[:2]
    length, inner = inputs_inner.shape[1:]
    own_width = inner_window.shape[2]
    states = pool_states.reshape(slots, -1, pool_states.shape[-1])
    rows = states.shape[1]

    capacity = (2 * slots + peers - 1) // peers
    index = jnp.arange(slots, dtype=jnp.int32)
    sides = 2
    parts = peers // sides
    side, seat = me // parts, lax.rem(me, parts)
    every = exchange(letters(move_plan, active_mask, inner_window, state_window, peers, capacity))
    packed = pack_pieces(states, active_mask, parts)
    packed, every = lax.optimization_barrier((packed, every))
    groups = [list(range(z * parts, (z + 1) * parts)) for z in range(sides)]
    got = lax.all_to_all(packed, "req", 0, 0, axis_index_groups=groups, tiled=True)
    got = got.reshape((parts * slots,) + got.shape[2:])

    def hop(value, across, by):
        pairs = [
            (z * parts + q, ((z + across) % sides) * parts + (q + by) % parts) for z in range(sides) for q in range(parts)
        ]
        return lax.ppermute(value, "req", pairs)

    taps = KERNEL - 1
    outer_own = state_window.shape[2]
    every_plan = every[:, taps * capacity, : 3 * slots].astype(jnp.int32)
    x, xs = inputs_inner[0], inputs_state[0]
    tail = jnp.concatenate([x[length - taps :], xs[length - taps :]], axis=1)
    to_me = every_plan[:, :slots] == me
    wanted = to_me & (every_plan[:, slots : 2 * slots] == 0)
    head_rank = jnp.sum(jnp.where(to_me & (index < jnp.sum(jnp.where(wanted, index, 0))), 1, 0) * jnp.any(wanted, axis=1, keepdims=True))
    head_peer = jnp.sum(jnp.where(wanted, jnp.arange(peers, dtype=jnp.int32)[:, None], 0))
    head_boxes = lax.dynamic_index_in_dim(every, head_peer, 0, keepdims=False)
    head = lax.dynamic_slice_in_dim(head_boxes, head_rank * taps, taps, 0)[:, : own_width + outer_own]

    positions = rank * length + jnp.arange(length, dtype=jnp.int32)
    steps = jax.nn.softplus(step_raw[0].astype(jnp.float32) + step_bias) * (positions < lengths[0])[:, None]
    own_decay = jnp.exp(jnp.sum(steps * -jnp.exp(decay_log), axis=0))
    digits, left = [], own_decay
    for _ in range(taps):
        digits.append(left.astype(jnp.bfloat16))
        left = left - digits[-1].astype(jnp.float32)
    edges = lax.all_gather(jnp.concatenate([tail, head, jnp.stack(digits)], axis=1), "seq")
    decays = jnp.sum(edges[:, :, tail.shape[1] + head.shape[1] :].astype(jnp.float32), axis=1)
    near_table, far_table, first_table, info, own_box, needed = tables(
        jnp.stack([me, side, seat]).astype(jnp.int32), every_plan, peers, parts, slots, capacity
    )
    before = lax.dynamic_index_in_dim(edges, lax.rem(rank + chain - 1, chain), 0, keepdims=False)[:, : tail.shape[1]]
    head = edges[:, :, tail.shape[1] : tail.shape[1] + head.shape[1]]
    head_inner = jnp.moveaxis(head[:, :, :own_width], 0, 1).reshape(taps, -1)
    head_outer = jnp.moveaxis(head[:, :, own_width:], 0, 1).reshape(taps, -1)
    window = jnp.where(rank == 0, jnp.concatenate([head_inner, head_outer], axis=1), before)
    window = jnp.pad(window.astype(jnp.float32), ((HALO - taps, 0), (0, 0)))

    valid_count = (lengths - rank * length).astype(jnp.int32)
    skip_row = jnp.repeat(skip_weight, HEAD_DIM)[None]
    seqs = jnp.arange(chain)
    coef, second_rows = [], []
    group = jnp.ones_like(decays[0])
    step = 1
    while step < chain:
        upper = (rank // step) % 2
        base = (rank // (2 * step)) * (2 * step)
        second = (seqs >= base + step) & (seqs < base + 2 * step)
        first_half = (seqs >= base) & (seqs < base + step)
        second_rows.append(jnp.prod(jnp.where(second[:, None], decays, 1.0), axis=0))
        coef.append(jnp.where(upper == 1, group, 0.0))
        group = jnp.where(upper == 1, group * jnp.prod(jnp.where(first_half[:, None], decays, 1.0), axis=0), group)
        step *= 2
    levels = len(coef)
    factors = jnp.repeat(jnp.stack(coef + [group] + second_rows + [jnp.prod(decays, axis=0)]), HEAD_DIM, axis=1)
    whole_own = lax.dynamic_slice_in_dim(factors[2 * levels + 1 :], rank * own_width, own_width, 1)

    def arrive(
        limit, got, first_table, near_table, far_table, info, own_box, every, x, xs, window, factors, whole_own, valid_count,
        conv_weight, conv_bias, step_raw, skip_row, gate, norm,
    ):
        first, token = sort_pieces(first_table, got, peers)
        first = exchange(first[0])
        far_all, token = sort_pieces(far_table + token, got, limit)
        far = [hop(far_all[m], 1, m) for m in range(parts)]
        near_all, token = sort_pieces(near_table + token, got, slots - 1)
        near = [near_all[0]] + [hop(near_all[m], 0, m) for m in range(1, parts)]
        part, end, ecum, read = mix(
            valid_count + token, x, xs, window, conv_weight, conv_bias, step_raw, step_bias, decay_log, skip_row
        )
        ends, total = [], end
        step = 1
        for level in range(levels):
            if level == 1:
                odd, width = rank % 2, inner // 2
                part_came = flip(lax.dynamic_slice_in_dim(total, odd * width, width, 1), "seq", step)
                part_other = flip(part_came, "seq", 1)
                came_end = jnp.concatenate(
                    [jnp.where(odd == 0, part_came, part_other), jnp.where(odd == 0, part_other, part_came)], axis=1
                )
            else:
                came_end = flip(total, "seq", step)
            upper = (rank // step) % 2
            ends.append(came_end)
            row = factors[levels + 1 + level][None]
            low, high = jnp.where(upper == 1, came_end, total), jnp.where(upper == 1, total, came_end)
            step *= 2
            if step < chain:
                total = (row * low.astype(jnp.float32) + high.astype(jnp.float32)).astype(jnp.bfloat16)
            else:
                own = lambda array: lax.dynamic_slice_in_dim(array, rank * own_width, own_width, 1)
                final = own(row) * own(low).astype(jnp.float32) + own(high).astype(jnp.float32)
        after = (total[0, 0].astype(jnp.float32) * 0.0).astype(jnp.int32)
        kind = info[0, 0]
        initial_own = lax.dynamic_slice_in_dim(first, jnp.where(kind == 1, side, 1 - side) * parts, parts, 0).reshape(rows, -1)
        initial_own = jnp.where(kind > 0, initial_own, jnp.zeros_like(initial_own))
        initial = jnp.stack(by_mask(initial_own, "seq"))
        out, token = finish(
            jnp.concatenate([valid_count, rank[None]]), part, gate, read, ecum, ends, factors, initial, norm
        )
        placed = land(info, final, whole_own, initial_own, near, far)
        position = lengths[0] + after - taps + jnp.arange(taps, dtype=jnp.int32) - rank * length
        inside = (position >= 0) & (position < length)
        clipped = jnp.clip(position, 0, length - 1)
        last = jnp.concatenate([jnp.take(x, clipped, axis=0), jnp.take(xs, clipped, axis=0)], axis=1)
        last = jnp.where(inside[:, None], last, jnp.zeros_like(last))
        kept = sum(piece.astype(jnp.float32) for piece in by_mask(last, "seq")).astype(jnp.bfloat16)
        kept_inner = lax.dynamic_slice_in_dim(kept, rank * own_width, own_width, 1)
        kept_outer = lax.dynamic_slice_in_dim(kept, inner + rank * outer_own, outer_own, 1)
        came = every[:, : taps * capacity].reshape(peers * capacity, taps, -1)
        moved = jnp.take(came, own_box[1:] + after, axis=0)
        new_inner = jnp.concatenate([kept_inner[None], moved[:, :, :own_width]], axis=0)
        new_outer = jnp.concatenate([kept_outer[None], moved[:, :, own_width : own_width + outer_own]], axis=0)
        return placed, out, new_inner, new_outer

    limits = sorted({min(slots - 1, limit) for limit in LIMITS} | {slots - 1})
    pick = sum((needed[0] > limit).astype(jnp.int32) for limit in limits[:-1])
    placed, out, new_inner, new_outer = lax.switch(
        pick, [functools.partial(arrive, limit) for limit in limits],
        got, first_table, near_table, far_table, info, own_box, every, x, xs, window, factors, whole_own, valid_count,
        conv_weight, conv_bias, step_raw[0], skip_row, gate_rows[0], norm_weight[None],
    )
    return (placed.reshape(pool_states.shape), new_inner, new_outer, out[None])


def solution(mesh):
    return jax.shard_map(
        on_device,
        mesh=mesh,
        in_specs=(
            P("req", "seq", None, None), P("req", None, "seq"), P("req", None, "seq"), P("req", None), P("req"),
            P("req", "seq", None), P("req", "seq", None), P("req", "seq", None), P("req", "seq", None), P("req"),
            P(), P(), P(), P(), P(), P(),
        ),
        out_specs=(
            P("req", "seq", None, None), P("req", None, "seq"), P("req", None, "seq"), P("req", "seq", None),
        ),
        check_vma=False,
    )
```

```python
import functools

import jax
import jax.numpy as jnp
from jax import lax
from jax.experimental import pallas as pl
from jax.experimental.pallas import tpu as pltpu
from jax.sharding import PartitionSpec as P


HEAD_DIM = 64
STATE_DIM = 128
KERNEL = 4
BLOCK_LEN = 256
EPSILON = 1e-05
LANES = 128
HALO = 8
LOG2E = 1.4426950408889634
GROUP = 2 * LANES


def half_silu(v):
    return (0.5 * v) * (1.0 + jnp.tanh(0.5 * v))


def conv_rows(ext_ref, weight_ref, bias_ref, start, count):
    total = bias_ref[...] + weight_ref[KERNEL - 1 : KERNEL, :] * ext_ref[pl.ds(start + HALO, count), :]
    for k in range(KERNEL - 1):
        total = total + weight_ref[k : k + 1, :] * ext_ref[pl.ds(start + HALO - KERNEL + 1 + k, count), :]
    return half_silu(total).astype(jnp.bfloat16)


def mix_kernel(
    nv_ref, x_ref, win_ref, cw_ref, cb_ref, skip_ref, xs_ref, wins_ref, cws_ref, cbs_ref, step_ref, sbias_ref, dlog_ref,
    part_ref, end_ref, ecum_ref, read_ref,
    ext, val, a_s, te_s, brow, write_t, score,
):
    g = pl.program_id(0)
    length = x_ref.shape[0]
    blocks = length // BLOCK_LEN
    half = BLOCK_LEN // 2

    @pl.when(g == 0)
    def _():
        ext[0:HALO, :] = wins_ref[...].astype(jnp.float32)
        ext[HALO : HALO + length, :] = xs_ref[...].astype(jnp.float32)
        ys = conv_rows(ext, cws_ref, cbs_ref, 0, length)
        write, read = ys[:, :STATE_DIM], ys[:, STATE_DIM:]
        read_ref[...] = read
        write_t[...] = write.astype(jnp.float32).T.astype(jnp.bfloat16)
        rows = lax.broadcasted_iota(jnp.int32, (length, LANES), 0)
        raw = step_ref[...] + sbias_ref[...]
        soft = jnp.maximum(raw, 0.0) + jnp.log1p(jnp.exp(-jnp.abs(raw)))
        dt = jnp.where(rows < nv_ref[0], soft, 0.0)
        rate = (dt * LOG2E) * (-jnp.exp(dlog_ref[...]))
        r = lax.broadcasted_iota(jnp.int32, (BLOCK_LEN, BLOCK_LEN), 0)
        c = lax.broadcasted_iota(jnp.int32, (BLOCK_LEN, BLOCK_LEN), 1)
        tri = (r >= c).astype(jnp.float32)
        before = jnp.zeros((1, LANES), jnp.float32)
        for blk in range(blocks):
            s = slice(blk * BLOCK_LEN, (blk + 1) * BLOCK_LEN)
            cum = jnp.dot(tri, rate[s], precision=lax.Precision.HIGHEST, preferred_element_type=jnp.float32)
            b = jnp.where(dt[s] > 0.0, cum - jnp.log2(dt[s]), 1e30)
            a_s[s, :] = cum
            last = cum[BLOCK_LEN - 1 : BLOCK_LEN, :]
            te_s[s, :] = jnp.exp2(last - b)
            brow[:, s] = b.T
            ecum_ref[s, :] = jnp.exp2(cum + before)
            before = before + last
            sc = lax.dot_general(read[s], write[s], (((1,), (1,)), ((), ())), preferred_element_type=jnp.float32)
            score[blk] = jnp.where(r >= c, sc, 0.0)

    ext[0:HALO, :] = win_ref[...].astype(jnp.float32)
    ext[HALO : HALO + length, :] = x_ref[...].astype(jnp.float32)
    rows_at_once = 64
    for i in range(length // rows_at_once):
        val[i * rows_at_once : (i + 1) * rows_at_once, :] = conv_rows(ext, cw_ref, cb_ref, i * rows_at_once, rows_at_once)

    heads_step = GROUP // HEAD_DIM
    turn = lax.rem(LANES - heads_step * g, LANES)
    a_all = pltpu.roll(a_s[...], turn, axis=1)
    te_all = pltpu.roll(te_s[...], turn, axis=1)
    low = lax.broadcasted_iota(jnp.int32, (1, LANES), 1) < HEAD_DIM

    for pair in range(GROUP // LANES):
        cols = slice(pair * LANES, (pair + 1) * LANES)
        skip = skip_ref[:, cols]
        before = None
        for blk in range(blocks):
            s = slice(blk * BLOCK_LEN, (blk + 1) * BLOCK_LEN)
            v = val[s, cols]
            vf = v.astype(jnp.float32)
            masked = [jnp.where(low, vf, 0.0).astype(jnp.bfloat16), jnp.where(low, 0.0, vf).astype(jnp.bfloat16)]
            tops, bottoms = [], []
            for j in range(2):
                h = 2 * pair + j
                a = a_all[s, h : h + 1]
                b = brow[pl.ds(heads_step * g + h, 1), s]
                top = jnp.exp2(jnp.minimum(a[:half] - b[:, :half], 126.0)) * score[blk, :half, :half]
                bot = jnp.exp2(jnp.minimum(a[half:] - b, 126.0)) * score[blk, half:, :]
                tops.append(top.astype(jnp.bfloat16))
                bottoms.append(bot.astype(jnp.bfloat16))
            intra_top = jnp.dot(
                jnp.concatenate(tops, axis=1), jnp.concatenate([m[:half] for m in masked], axis=0), preferred_element_type=jnp.float32
            )
            intra_bot = jnp.dot(
                jnp.concatenate(bottoms, axis=1), jnp.concatenate(masked, axis=0), preferred_element_type=jnp.float32
            )
            out = jnp.concatenate([intra_top, intra_bot], axis=0) + skip * vf
            h = 2 * pair
            te = jnp.where(low, te_all[s, h : h + 1], te_all[s, h + 1 : h + 2])
            state = jnp.dot(write_t[:, s], (te * vf).astype(jnp.bfloat16), preferred_element_type=jnp.float32)
            if blk > 0:
                e = jnp.exp2(jnp.where(low, a_all[s, h : h + 1], a_all[s, h + 1 : h + 2]))
                out = out + e * jnp.dot(read_ref[s, :], before.astype(jnp.bfloat16), preferred_element_type=jnp.float32)
                state = state + e[BLOCK_LEN - 1 : BLOCK_LEN, :] * before
            before = state
            part_ref[s, cols] = out.astype(jnp.bfloat16)
        end_ref[:, cols] = before.astype(jnp.bfloat16)


def mix(nv, x, xs, window, conv_weight, conv_bias, step_raw, step_bias, decay_log, skip_row):
    length, inner = x.shape
    pad = LANES - step_raw.shape[1]
    step = jnp.pad(step_raw.astype(jnp.float32), ((0, 0), (0, pad)))
    sbias = jnp.pad(step_bias, (0, pad))[None]
    dlog = jnp.pad(decay_log, (0, pad))[None]
    xs_width = xs.shape[1]
    beyond = inner // xs_width
    state_column = lambda rows: pl.BlockSpec((rows, xs_width), lambda i, nv: (0, beyond))
    fixed = lambda shape: pl.BlockSpec(shape, lambda i, nv: (0,) * len(shape))
    column = lambda rows: pl.BlockSpec((rows, GROUP), lambda i, nv: (0, i))
    blocks = length // BLOCK_LEN
    heads = inner // HEAD_DIM
    return pl.pallas_call(
        mix_kernel,
        grid_spec=pltpu.PrefetchScalarGridSpec(
            num_scalar_prefetch=1,
            grid=(inner // GROUP,),
            in_specs=[
                column(length), column(HALO), column(KERNEL), column(1), column(1),
                fixed((length, xs_width)), state_column(HALO), state_column(KERNEL), state_column(1),
                fixed((length, LANES)), fixed((1, LANES)), fixed((1, LANES)),
            ],
            out_specs=[column(length), column(STATE_DIM), fixed((length, LANES)), fixed((length, STATE_DIM))],
            scratch_shapes=[
                pltpu.VMEM((length + HALO, GROUP), jnp.float32),
                pltpu.VMEM((length, GROUP), jnp.bfloat16),
                pltpu.VMEM((length, LANES), jnp.float32),
                pltpu.VMEM((length, LANES), jnp.float32),
                pltpu.VMEM((LANES, length), jnp.float32),
                pltpu.VMEM((STATE_DIM, length), jnp.bfloat16),
                pltpu.VMEM((blocks, BLOCK_LEN, BLOCK_LEN), jnp.float32),
            ],
        ),
        out_shape=[
            jax.ShapeDtypeStruct((length, inner), jnp.bfloat16),
            jax.ShapeDtypeStruct((STATE_DIM, inner), jnp.bfloat16),
            jax.ShapeDtypeStruct((length, LANES), jnp.float32),
            jax.ShapeDtypeStruct((length, STATE_DIM), jnp.bfloat16),
        ],
        compiler_params=pltpu.CompilerParams(dimension_semantics=("arbitrary",)),
        cost_estimate=pl.CostEstimate(
            flops=2 * blocks * heads * BLOCK_LEN * BLOCK_LEN * LANES * 8,
            bytes_accessed=4 * length * inner, transcendentals=blocks * heads * BLOCK_LEN * BLOCK_LEN,
        ),
        name="mix",
    )(
        nv, x, window, conv_weight, conv_bias[None], skip_row, xs, window, conv_weight, conv_bias[None], step, sbias, dlog,
    )


CHUNK = 256


def finish_kernel(
    nv_ref, part_ref, gate_ref, read_ref, ecum_ref, coef_ref, init_ref, norm_ref, *refs
):
    out_ref, token_ref, prior, spread, gated = refs[-5:]
    ends_refs = refs[:-5]
    token_ref[0] = 0
    step = pl.program_id(0)
    tile, inner = part_ref.shape
    links = len(ends_refs)
    own_width = init_ref.shape[1]
    heads = inner // HEAD_DIM

    @pl.when(step == 0)
    def _():
        def fill(i, carry):
            cols = pl.ds(pl.multiple_of(i * CHUNK, CHUNK), CHUNK)
            total = coef_ref[0:1, cols] * ends_refs[0][:, cols].astype(jnp.float32)
            for j in range(1, links):
                total = total + coef_ref[j : j + 1, cols] * ends_refs[j][:, cols].astype(jnp.float32)
            prior[:, cols] = total.astype(jnp.bfloat16)
            k = lax.broadcasted_iota(jnp.int32, (LANES, CHUNK), 0)
            c = lax.broadcasted_iota(jnp.int32, (LANES, CHUNK), 1)
            owner = i * (CHUNK // HEAD_DIM) + c // HEAD_DIM
            spread[:, cols] = jnp.where((k == owner) | (k == owner + heads), 1.0, 0.0).astype(jnp.bfloat16)
            return carry

        lax.fori_loop(0, inner // CHUNK, fill, 0)

    read = read_ref[...]
    ecum = ecum_ref[...]
    first = ecum.astype(jnp.bfloat16).astype(jnp.float32)
    lane = lax.broadcasted_iota(jnp.int32, (tile, LANES), 1)
    both = jnp.where(lane < heads, first, pltpu.roll(ecum - first, heads, axis=1)).astype(jnp.bfloat16)
    rows = lax.broadcasted_iota(jnp.int32, (tile, 1), 0) + step * tile
    valid = (rows < nv_ref[0]).astype(jnp.float32)

    def gate_chunk(i, squares):
        cols = pl.ds(pl.multiple_of(i * CHUNK, CHUNK), CHUNK)
        z = jnp.dot(read, prior[:, cols], preferred_element_type=jnp.float32)
        chunks = own_width // CHUNK
        turned = nv_ref[1] ^ (i // chunks)
        own = init_ref[turned, pl.ds(pl.multiple_of(lax.rem(i, chunks) * CHUNK, CHUNK), CHUNK), :]
        zi = lax.dot_general(read, own, (((1,), (1,)), ((), ())), preferred_element_type=jnp.float32)
        e = jnp.dot(both, spread[:, cols], preferred_element_type=jnp.float32)
        z = z + coef_ref[links : links + 1, cols] * zi
        y = (part_ref[:, cols].astype(jnp.float32) + e * z) * valid
        y = y.astype(jnp.bfloat16).astype(jnp.float32)
        out = y * half_silu(gate_ref[:, cols].astype(jnp.float32))
        gated[:, cols] = out
        square = out * out
        for k in range(CHUNK // LANES):
            squares = squares + square[:, k * LANES : (k + 1) * LANES]
        return squares

    squares = lax.fori_loop(0, inner // CHUNK, gate_chunk, jnp.zeros((tile, LANES), jnp.float32), unroll=2)
    scale = lax.rsqrt(jnp.sum(squares, axis=1, keepdims=True) * (1.0 / inner) + EPSILON)

    def scale_chunk(i, carry):
        cols = pl.ds(pl.multiple_of(i * CHUNK, CHUNK), CHUNK)
        out_ref[:, cols] = (gated[:, cols] * scale * norm_ref[:, cols]).astype(jnp.bfloat16)
        return carry

    lax.fori_loop(0, inner // CHUNK, scale_chunk, 0, unroll=2)


def finish(nv, part, gate, read, ecum, ends, coef, initial, norm):
    length, inner = part.shape
    tile = min(128, length)
    fixed = lambda shape: pl.BlockSpec(shape, lambda i, nv: (0,) * len(shape))
    row = lambda width: pl.BlockSpec((tile, width), lambda i, nv: (i, 0))
    return pl.pallas_call(
        finish_kernel,
        grid_spec=pltpu.PrefetchScalarGridSpec(
            num_scalar_prefetch=1,
            grid=(length // tile,),
            in_specs=[
                row(inner), row(inner), row(STATE_DIM), row(LANES),
                fixed(coef.shape), fixed(initial.shape), fixed((1, inner)), *[fixed(e.shape) for e in ends],
            ],
            out_specs=[row(inner), pl.BlockSpec(memory_space=pltpu.SMEM)],
            scratch_shapes=[
                pltpu.VMEM((STATE_DIM, inner), jnp.bfloat16),
                pltpu.VMEM((LANES, inner), jnp.bfloat16),
                pltpu.VMEM((tile, inner), jnp.float32),
            ],
        ),
        out_shape=[jax.ShapeDtypeStruct((length, inner), jnp.bfloat16), jax.ShapeDtypeStruct((1,), jnp.int32)],
        compiler_params=pltpu.CompilerParams(dimension_semantics=("arbitrary",)),
        cost_estimate=pl.CostEstimate(
            flops=40 * length * inner * STATE_DIM // 8, bytes_accessed=6 * length * inner, transcendentals=length * inner
        ),
        name="finish",
    )(nv, part, gate, read, ecum, coef, initial, norm, *ends)


def pack_kernel(keep_ref, state_ref, out_ref, held, packed, in_sem, out_sem):
    peers, slots, rows, _ = out_ref.shape

    def load(j):
        return pltpu.make_async_copy(state_ref.at[j], held.at[j], in_sem.at[j])

    def store(j):
        return pltpu.make_async_copy(packed.at[j], out_ref.at[:, j], out_sem.at[j])

    def first(j, carry):
        load(j).start()
        return carry

    def second(j, carry):
        load(j).wait()
        keep = keep_ref[j].astype(jnp.float32)
        for i in range(peers):
            packed[j, i] = (held[j, i * rows : (i + 1) * rows] * keep).astype(packed.dtype)
        store(j).start()
        return carry

    def third(j, carry):
        store(j).wait()
        return carry

    lax.fori_loop(0, slots, first, 0)
    lax.fori_loop(0, slots, second, 0)
    lax.fori_loop(0, slots, third, 0)


def pack_pieces(states, keep, peers):
    slots, rows, lanes = states.shape
    piece = rows // peers
    return pl.pallas_call(
        pack_kernel,
        in_specs=[pl.BlockSpec(memory_space=pltpu.SMEM), pl.BlockSpec(memory_space=pl.ANY)],
        out_specs=pl.BlockSpec(memory_space=pl.ANY),
        out_shape=jax.ShapeDtypeStruct((peers, slots, piece, lanes), jnp.bfloat16),
        scratch_shapes=[
            pltpu.VMEM((slots, rows, lanes), jnp.float32),
            pltpu.VMEM((slots, peers, piece, lanes), jnp.bfloat16),
            pltpu.SemaphoreType.DMA((slots,)),
            pltpu.SemaphoreType.DMA((slots,)),
        ],
        cost_estimate=pl.CostEstimate(flops=20 * slots * rows * lanes, bytes_accessed=6 * slots * rows * lanes, transcendentals=0),
        name="pack",
    )(keep, states)


def letters_kernel(capacity, plan_ref, mask_ref, inner_ref, outer_ref, plan_row_ref, out_ref, table, count, wide_inner, wide_outer):
    taps, slots, inner = inner_ref.shape
    outer = outer_ref.shape[2]
    peers, rows, width = out_ref.shape
    wide_inner[...] = inner_ref[...].astype(jnp.float32)
    wide_outer[...] = outer_ref[...].astype(jnp.float32)

    def clear(d, carry):
        count[d] = 0
        for r in range(capacity):
            table[d * capacity + r] = -1
        return carry

    def enter(j, carry):
        d = plan_ref[0, j]
        table[d * capacity + count[d]] = jnp.where(mask_ref[j] != 0, j, -1)
        count[d] = count[d] + 1
        return carry

    lax.fori_loop(0, peers, clear, 0)
    lax.fori_loop(0, slots, enter, 0)

    def fill(d, carry):
        pieces = []
        for r in range(capacity):
            j = table[d * capacity + r]
            at = jnp.maximum(j, 0)
            for t in range(taps):
                row = jnp.concatenate(
                    [wide_inner[t, pl.ds(at, 1), :], wide_outer[t, pl.ds(at, 1), :], jnp.zeros((1, width - inner - outer), jnp.float32)],
                    axis=1,
                )
                pieces.append(jnp.where(j >= 0, row, 0.0))
        pieces.append(plan_row_ref[...])
        left = rows - taps * capacity - 1
        if left:
            pieces.append(jnp.zeros((left, width), jnp.float32))
        out_ref[d] = jnp.concatenate(pieces, axis=0).astype(out_ref.dtype)
        return carry

    lax.fori_loop(0, peers, fill, 0)


def letters(plan, mask, inner_window, outer_window, peers, capacity):
    slots, taps, inner = inner_window.shape
    outer = outer_window.shape[2]
    width = inner + outer
    width += -width % LANES
    rows = taps * capacity + 1
    rows += -rows % 16
    plan_row = jnp.concatenate([plan[:, 0], plan[:, 1], mask]).astype(jnp.float32)[None]
    plan_row = jnp.pad(plan_row, ((0, 0), (0, width - 3 * slots)))
    smem, vmem = pl.BlockSpec(memory_space=pltpu.SMEM), pl.BlockSpec(memory_space=pltpu.VMEM)
    return pl.pallas_call(
        functools.partial(letters_kernel, capacity),
        in_specs=[smem, smem, vmem, vmem, vmem],
        out_specs=vmem,
        out_shape=jax.ShapeDtypeStruct((peers, rows, width), jnp.bfloat16),
        scratch_shapes=[
            pltpu.SMEM((peers * capacity,), jnp.int32),
            pltpu.SMEM((peers,), jnp.int32),
            pltpu.VMEM((taps, slots, inner), jnp.float32),
            pltpu.VMEM((taps, slots, outer), jnp.float32),
        ],
        cost_estimate=pl.CostEstimate(flops=100000, bytes_accessed=8 * slots * taps * width, transcendentals=0),
        name="letters",
    )(plan.T, mask, jnp.moveaxis(inner_window, 1, 0), jnp.moveaxis(outer_window, 1, 0), plan_row)


def sort_kernel(sizes, turn_ref, *refs):
    tables, got_ref = refs[: len(sizes)], refs[len(sizes)]
    refs = refs[len(sizes) + 1 :]
    total = sum(parts for parts, _ in sizes)
    outs, token_ref = refs[:total], refs[total]
    stages, in_sem, out_sem = refs[total + 1 : total + 1 + len(sizes)], refs[-2], refs[-1]
    token_ref[0] = turn_ref[0]
    number = 0
    for (parts, count), table_ref, stage in zip(sizes, tables, stages):

        def one(k, carry, parts=parts, table_ref=table_ref, stage=stage, number=number):
            for m in range(parts):
                pltpu.make_async_copy(got_ref.at[table_ref[m, k]], stage.at[m, k], in_sem.at[number + m]).start()
            return carry

        lax.fori_loop(0, count, one, 0)
        number += parts
    copies = []
    for (parts, count), stage in zip(sizes, stages):
        for m in range(parts):
            pltpu.make_async_copy(got_ref.at[0:count], stage.at[m], in_sem.at[len(copies)]).wait()
            copies.append(pltpu.make_async_copy(stage.at[m], outs[len(copies)], out_sem.at[len(copies)]))
            copies[-1].start()
    for copy in copies:
        copy.wait()


def sort_pieces(turn, got, *jobs):
    rows, lanes = got.shape[1:]
    sizes = [(table.shape[0], count) for table, count in jobs]
    total = sum(parts for parts, _ in sizes)
    smem, whole = pl.BlockSpec(memory_space=pltpu.SMEM), pl.BlockSpec(memory_space=pl.ANY)
    work = sum(parts * count for parts, count in sizes) * rows * lanes
    outs = pl.pallas_call(
        functools.partial(sort_kernel, sizes),
        in_specs=[smem] * (1 + len(jobs)) + [whole],
        out_specs=[whole] * total + [smem],
        out_shape=[jax.ShapeDtypeStruct((count, rows, lanes), jnp.bfloat16) for parts, count in sizes for _ in range(parts)]
        + [jax.ShapeDtypeStruct((1,), jnp.int32)],
        scratch_shapes=[pltpu.VMEM((parts, count, rows, lanes), jnp.bfloat16) for parts, count in sizes]
        + [pltpu.SemaphoreType.DMA((total,)), pltpu.SemaphoreType.DMA((total,))],
        cost_estimate=pl.CostEstimate(flops=10 * work, bytes_accessed=4 * work, transcendentals=0),
        name="sort",
    )(turn, *[table for table, _ in jobs], got)
    return outs[:-1], outs[-1]


def tables_kernel(peers, parts, slots, capacity, place_ref, plan_ref, near_ref, far_ref, first_ref, info_ref, box_ref, need_ref, inverse):
    me, side, seat = place_ref[0], place_ref[1], place_ref[2]

    def one_source(r, carry):
        def one_slot(j, count):
            d, k = plan_ref[r, j], plan_ref[r, slots + j]
            inverse[d * slots + k] = (r << 9) + (j << 1) + plan_ref[r, 2 * slots + j]

            @pl.when(d == me)
            def _():
                box_ref[k] = r * capacity + count

            return count + (d == me).astype(jnp.int32)

        lax.fori_loop(0, slots, one_slot, 0)
        return carry

    def clear(k, carry):
        for m in range(parts):
            near_ref[m, k] = 0
            far_ref[m, k] = 0
        return carry

    lax.fori_loop(0, peers, one_source, 0)
    lax.fori_loop(0, slots - 1, clear, 0)

    def one_target(d, most):
        d_side = (d >= parts).astype(jnp.int32)
        m = lax.rem(d - d_side * parts + parts - seat, parts)

        def one_slot(k, count):
            code = inverse[d * slots + k]
            live = (code & 1) == 1
            r = code >> 9
            r_side = (r >= parts).astype(jnp.int32)
            held = (r - r_side * parts) * slots + ((code >> 1) & 255)
            far = live & (r_side != d_side)

            @pl.when(d == me)
            def _():
                info_ref[0, k] = jnp.where(live, jnp.where(far, jnp.where(count == 0, 3, 2), 1), 0)
                info_ref[1, k] = count - 1
                info_ref[2, k] = jnp.where(k == 0, 0, jnp.where(k == 1, seat, (1 - side) * parts))

            here = live & (r_side == side)

            @pl.when(here & ((far & (count == 0)) | ((k == 0) & ~far)))
            def _():
                first_ref[0, d] = held

            @pl.when(here & (k > 0) & ~far)
            def _():
                near_ref[m, k - 1] = held

            @pl.when(here & far & (count > 0))
            def _():
                far_ref[m, count - 1] = held

            return count + far.astype(jnp.int32)

        first_ref[0, d] = 0
        return jnp.maximum(most, lax.fori_loop(0, slots, one_slot, 0) - 1)

    need_ref[0] = lax.fori_loop(0, peers, one_target, 0)


def tables(place, plan, peers, parts, slots, capacity):
    smem = pl.BlockSpec(memory_space=pltpu.SMEM)
    ints = lambda *shape: jax.ShapeDtypeStruct(shape, jnp.int32)
    return pl.pallas_call(
        functools.partial(tables_kernel, peers, parts, slots, capacity),
        in_specs=[smem, smem],
        out_specs=[smem] * 6,
        out_shape=[ints(parts, slots - 1), ints(parts, slots - 1), ints(1, peers), ints(3, slots), ints(slots), ints(1)],
        scratch_shapes=[pltpu.SMEM((peers * slots,), jnp.int32)],
        cost_estimate=pl.CostEstimate(flops=1000000, bytes_accessed=4000, transcendentals=0),
        name="tables",
    )(place, plan)


def land_kernel(parts, info_ref, final_ref, whole_ref, initial_ref, first_ref, *refs):
    near, far = refs[:parts], refs[parts : 2 * parts]
    out_ref, held, wide, in_sem, out_sem = refs[2 * parts :]
    rest, rows, _ = near[0].shape
    slots = rest + 1

    def each(k, act):
        kind, at = info_ref[0, k], info_ref[1, k]

        @pl.when(kind == 1)
        def _():
            for m in range(parts):
                act(pltpu.make_async_copy(near[m].at[k - 1], held.at[k, m], in_sem.at[k]))

        @pl.when(kind == 2)
        def _():
            for m in range(parts):
                act(pltpu.make_async_copy(far[m].at[at], held.at[k, m], in_sem.at[k]))

        @pl.when(kind == 3)
        def _():
            for m in range(parts):
                sender = info_ref[2, 2] + lax.rem(info_ref[2, 1] + parts - m, parts)
                act(pltpu.make_async_copy(first_ref.at[sender], held.at[k, m], in_sem.at[k]))

    def store(k):
        return pltpu.make_async_copy(wide.at[k], out_ref.at[k], out_sem.at[k])

    def first(k, carry):
        each(k, lambda copy: copy.start())
        return carry

    def second(k, carry):
        each(k, lambda copy: copy.wait())
        kind = info_ref[0, k]
        for m in range(parts):
            begin = pl.multiple_of(lax.rem(info_ref[2, 1] + parts - m, parts) * rows, rows)
            wide[k, pl.ds(begin, rows)] = jnp.where(kind > 0, held[k, m].astype(wide.dtype), 0.0)
        store(k).start()
        return carry

    def third(k, carry):
        store(k).wait()
        return carry

    lax.fori_loop(1, slots, first, 0)
    for i in range(0, final_ref.shape[1], LANES):
        own = slice(i, i + LANES)
        moved = initial_ref[own, :].astype(jnp.float32).T
        wide[0, own, :] = (final_ref[:, own] + whole_ref[:, own] * moved).T
    store(0).start()
    lax.fori_loop(1, slots, second, 0)
    lax.fori_loop(0, slots, third, 0)


def land(info, final, whole_own, initial_own, first, near, far):
    parts = len(near)
    rest, rows, lanes = near[0].shape
    slots = rest + 1
    smem, vmem, whole = (pl.BlockSpec(memory_space=space) for space in (pltpu.SMEM, pltpu.VMEM, pl.ANY))
    return pl.pallas_call(
        functools.partial(land_kernel, parts),
        in_specs=[smem, vmem, vmem, vmem] + [whole] * (2 * parts + 1),
        out_specs=whole,
        out_shape=jax.ShapeDtypeStruct((slots, parts * rows, lanes), jnp.float32),
        scratch_shapes=[
            pltpu.VMEM((slots, parts, rows, lanes), jnp.bfloat16),
            pltpu.VMEM((slots, parts * rows, lanes), jnp.float32),
            pltpu.SemaphoreType.DMA((slots,)),
            pltpu.SemaphoreType.DMA((slots,)),
        ],
        cost_estimate=pl.CostEstimate(
            flops=20 * slots * parts * rows * lanes, bytes_accessed=6 * slots * parts * rows * lanes, transcendentals=0
        ),
        name="land",
    )(info, final, whole_own, initial_own, first, *near, *far)


def exchange(source):
    return lax.all_to_all(source, "req", split_axis=0, concat_axis=0, tiled=True)


def flip(value, axis, step):
    return lax.ppermute(value, axis, [(r, r ^ step) for r in range(lax.axis_size(axis))])


def by_mask(value, axis):
    held, step = {0: value}, lax.axis_size(axis) // 2
    while step:
        masks = sorted(held)
        came = flip(jnp.stack([held[m] for m in masks]) if len(masks) > 1 else held[masks[0]][None], axis, step)
        held.update({m ^ step: came[i] for i, m in enumerate(masks)})
        step //= 2
    return [held[m] for m in sorted(held)]


LIMITS = (8, 10)


def on_device(
    pool_states, inner_window, state_window, move_plan, active_mask, inputs_inner, inputs_state, gate_rows, step_raw,
    lengths, conv_weight, conv_bias, step_bias, decay_log, skip_weight, norm_weight,
):
    peers, me = lax.axis_size("req"), lax.axis_index("req")
    chain, rank = lax.axis_size("seq"), lax.axis_index("seq")
    slots, _ = pool_states.shape[:2]
    length, inner = inputs_inner.shape[1:]
    own_width = inner_window.shape[2]
    states = pool_states.reshape(slots, -1, pool_states.shape[-1])
    rows = states.shape[1]

    capacity = (2 * slots + peers - 1) // peers
    index = jnp.arange(slots, dtype=jnp.int32)
    sides = 2
    parts = peers // sides
    side, seat = me // parts, lax.rem(me, parts)
    every = exchange(letters(move_plan, active_mask, inner_window, state_window, peers, capacity))
    packed = pack_pieces(states, active_mask, parts)
    packed, every = lax.optimization_barrier((packed, every))
    groups = [list(range(z * parts, (z + 1) * parts)) for z in range(sides)]
    got = lax.all_to_all(packed, "req", 0, 0, axis_index_groups=groups, tiled=True)
    got = got.reshape((parts * slots,) + got.shape[2:])

    def hop(value, across, by):
        pairs = [
            (z * parts + q, ((z + across) % sides) * parts + (q + by) % parts) for z in range(sides) for q in range(parts)
        ]
        return lax.ppermute(value, "req", pairs)

    taps = KERNEL - 1
    outer_own = state_window.shape[2]
    every_plan = every[:, taps * capacity, : 3 * slots].astype(jnp.int32)
    x, xs = inputs_inner[0], inputs_state[0]
    tail = jnp.concatenate([x[length - taps :], xs[length - taps :]], axis=1)
    to_me = every_plan[:, :slots] == me
    wanted = to_me & (every_plan[:, slots : 2 * slots] == 0)
    head_rank = jnp.sum(jnp.where(to_me & (index < jnp.sum(jnp.where(wanted, index, 0))), 1, 0) * jnp.any(wanted, axis=1, keepdims=True))
    head_peer = jnp.sum(jnp.where(wanted, jnp.arange(peers, dtype=jnp.int32)[:, None], 0))
    head_boxes = lax.dynamic_index_in_dim(every, head_peer, 0, keepdims=False)
    head = lax.dynamic_slice_in_dim(head_boxes, head_rank * taps, taps, 0)[:, : own_width + outer_own]

    positions = rank * length + jnp.arange(length, dtype=jnp.int32)
    steps = jax.nn.softplus(step_raw[0].astype(jnp.float32) + step_bias) * (positions < lengths[0])[:, None]
    own_decay = jnp.exp(jnp.sum(steps * -jnp.exp(decay_log), axis=0))
    digits, left = [], own_decay
    for _ in range(taps):
        digits.append(left.astype(jnp.bfloat16))
        left = left - digits[-1].astype(jnp.float32)
    edges = lax.all_gather(jnp.concatenate([tail, head, jnp.stack(digits)], axis=1), "seq")
    decays = jnp.sum(edges[:, :, tail.shape[1] + head.shape[1] :].astype(jnp.float32), axis=1)
    near_table, far_table, first_table, info, own_box, needed = tables(
        jnp.stack([me, side, seat]).astype(jnp.int32), every_plan, peers, parts, slots, capacity
    )
    before = lax.dynamic_index_in_dim(edges, lax.rem(rank + chain - 1, chain), 0, keepdims=False)[:, : tail.shape[1]]
    head = edges[:, :, tail.shape[1] : tail.shape[1] + head.shape[1]]
    head_inner = jnp.moveaxis(head[:, :, :own_width], 0, 1).reshape(taps, -1)
    head_outer = jnp.moveaxis(head[:, :, own_width:], 0, 1).reshape(taps, -1)
    window = jnp.where(rank == 0, jnp.concatenate([head_inner, head_outer], axis=1), before)
    window = jnp.pad(window.astype(jnp.float32), ((HALO - taps, 0), (0, 0)))

    valid_count = (lengths - rank * length).astype(jnp.int32)
    skip_row = jnp.repeat(skip_weight, HEAD_DIM)[None]
    seqs = jnp.arange(chain)
    coef, second_rows = [], []
    group = jnp.ones_like(decays[0])
    step = 1
    while step < chain:
        upper = (rank // step) % 2
        base = (rank // (2 * step)) * (2 * step)
        second = (seqs >= base + step) & (seqs < base + 2 * step)
        first_half = (seqs >= base) & (seqs < base + step)
        second_rows.append(jnp.prod(jnp.where(second[:, None], decays, 1.0), axis=0))
        coef.append(jnp.where(upper == 1, group, 0.0))
        group = jnp.where(upper == 1, group * jnp.prod(jnp.where(first_half[:, None], decays, 1.0), axis=0), group)
        step *= 2
    levels = len(coef)
    factors = jnp.repeat(jnp.stack(coef + [group] + second_rows + [jnp.prod(decays, axis=0)]), HEAD_DIM, axis=1)
    whole_own = lax.dynamic_slice_in_dim(factors[2 * levels + 1 :], rank * own_width, own_width, 1)

    def arrive(
        limit, got, first_table, near_table, far_table, info, own_box, every, x, xs, window, factors, whole_own, valid_count,
        conv_weight, conv_bias, step_raw, skip_row, gate, norm,
    ):
        sorted_pieces, token = sort_pieces(jnp.zeros((1,), jnp.int32), got, (first_table, peers), (far_table, limit))
        first = exchange(sorted_pieces[0])
        far = [hop(sorted_pieces[1 + m], 1, m) for m in range(parts)]
        near_all, token = sort_pieces(token, got, (near_table, slots - 1))
        near = [near_all[0]] + [hop(near_all[m], 0, m) for m in range(1, parts)]
        part, end, ecum, read = mix(
            valid_count + token[0], x, xs, window, conv_weight, conv_bias, step_raw, step_bias, decay_log, skip_row
        )
        ends, total = [], end
        step = 1
        for level in range(levels):
            if level == 1:
                odd, width = rank % 2, inner // 2
                part_came = flip(lax.dynamic_slice_in_dim(total, odd * width, width, 1), "seq", step)
                part_other = flip(part_came, "seq", 1)
                came_end = jnp.concatenate(
                    [jnp.where(odd == 0, part_came, part_other), jnp.where(odd == 0, part_other, part_came)], axis=1
                )
            else:
                came_end = flip(total, "seq", step)
            upper = (rank // step) % 2
            ends.append(came_end)
            row = factors[levels + 1 + level][None]
            low, high = jnp.where(upper == 1, came_end, total), jnp.where(upper == 1, total, came_end)
            step *= 2
            if step < chain:
                total = (row * low.astype(jnp.float32) + high.astype(jnp.float32)).astype(jnp.bfloat16)
            else:
                own = lambda array: lax.dynamic_slice_in_dim(array, rank * own_width, own_width, 1)
                final = own(row) * own(low).astype(jnp.float32) + own(high).astype(jnp.float32)
        after = (total[0, 0].astype(jnp.float32) * 0.0).astype(jnp.int32)
        kind = info[0, 0]
        initial_own = lax.dynamic_slice_in_dim(first, jnp.where(kind == 1, side, 1 - side) * parts, parts, 0).reshape(rows, -1)
        initial_own = jnp.where(kind > 0, initial_own, jnp.zeros_like(initial_own))
        initial = jnp.stack(by_mask(initial_own, "seq"))
        out, token = finish(
            jnp.concatenate([valid_count, rank[None]]), part, gate, read, ecum, ends, factors, initial, norm
        )
        placed = land(info, final, whole_own, initial_own, first, near, far)
        position = lengths[0] + after - taps + jnp.arange(taps, dtype=jnp.int32) - rank * length
        inside = (position >= 0) & (position < length)
        clipped = jnp.clip(position, 0, length - 1)
        last = jnp.concatenate([jnp.take(x, clipped, axis=0), jnp.take(xs, clipped, axis=0)], axis=1)
        last = jnp.where(inside[:, None], last, jnp.zeros_like(last))
        kept = sum(piece.astype(jnp.float32) for piece in by_mask(last, "seq")).astype(jnp.bfloat16)
        kept_inner = lax.dynamic_slice_in_dim(kept, rank * own_width, own_width, 1)
        kept_outer = lax.dynamic_slice_in_dim(kept, inner + rank * outer_own, outer_own, 1)
        came = every[:, : taps * capacity].reshape(peers * capacity, taps, -1)
        moved = jnp.take(came, own_box[1:] + after, axis=0)
        new_inner = jnp.concatenate([kept_inner[None], moved[:, :, :own_width]], axis=0)
        new_outer = jnp.concatenate([kept_outer[None], moved[:, :, own_width : own_width + outer_own]], axis=0)
        return placed, out, new_inner, new_outer

    limits = sorted({min(slots - 1, limit) for limit in LIMITS} | {slots - 1})
    pick = sum((needed[0] > limit).astype(jnp.int32) for limit in limits[:-1])
    placed, out, new_inner, new_outer = lax.switch(
        pick, [functools.partial(arrive, limit) for limit in limits],
        got, first_table, near_table, far_table, info, own_box, every, x, xs, window, factors, whole_own, valid_count,
        conv_weight, conv_bias, step_raw[0], skip_row, gate_rows[0], norm_weight[None],
    )
    return (placed.reshape(pool_states.shape), new_inner, new_outer, out[None])


def solution(mesh):
    return jax.shard_map(
        on_device,
        mesh=mesh,
        in_specs=(
            P("req", "seq", None, None), P("req", None, "seq"), P("req", None, "seq"), P("req", None), P("req"),
            P("req", "seq", None), P("req", "seq", None), P("req", "seq", None), P("req", "seq", None), P("req"),
            P(), P(), P(), P(), P(), P(),
        ),
        out_specs=(
            P("req", "seq", None, None), P("req", None, "seq"), P("req", None, "seq"), P("req", "seq", None),
        ),
        check_vma=False,
    )
```
